32 devices in a mesh: px: 4 (over y, x), py: 8 (over z, core).
Axes of the slice: x: 2, y: 2, z: 4, core: 2. Of those that a mesh axis runs over, the one named last changes fastest.
Arguments:
- coefficients: bfloat16 [384, 12288], P(('px', 'py')), may hold values from -6 to 6
- exponents: int32 [96, 768], P(('px', 'py')), may hold values from -4 to 1
- right_side: float32 [64, 192, 384], P('px', 'py'), may hold values from -18 to 18
Outputs:
- decoded: float32 [64, 192, 384], P('px', 'py')
- residual: float32 [64, 192, 384], P('px', 'py')
- rms: float32 [], replicated
The draws below stay inside these ranges and needn't reach their ends.
All inputs are finite; a program needn't handle non-finite values.
Results may differ from the reference program's by a relative error of at most 0.0003.
Values may be sent and summed in bfloat16 or wider, within the bound.
No kernel may reach another device: no remote copies, remote signals or barrier semaphores. Data moves between devices by JAX's collectives and lax.ppermute only.
A program may use at most 64 MiB of HBM per device.

```python
import jax
import jax.numpy as jnp
from jax import lax

CX = 16
CY = 24
BX = 16
BY = 48
BZ = 96
NX = 64
NY = 192
NZ = 384


def draw_exponents(key, part):
    block_x = CX // 4
    block_y = CY // 4
    pencil_x = BX // block_x
    pencil_y = BY // block_y
    drawn_levels = jax.random.randint(key, (BZ, pencil_x, pencil_y, block_x, block_y), -3, 1)
    across_x = jnp.arange(pencil_x, dtype=jnp.int32)[:, None] * block_x + jnp.arange(block_x, dtype=jnp.int32)[None, :]
    across_y = jnp.arange(pencil_y, dtype=jnp.int32)[:, None] * block_y + jnp.arange(block_y, dtype=jnp.int32)[None, :]
    slope_x = (2 * across_x // BX)[None, :, None, :, None]
    slope_y = (2 * across_y // BY)[None, None, :, None, :]
    levels = drawn_levels + slope_x + slope_y - 1
    return levels.reshape(BZ, BX * BY).astype(jnp.int32)


def draw_right_side(key, part):
    first_key, second_key = jax.random.split(jax.random.fold_in(key, 7))
    column_scale = 0.3 * jnp.exp(jax.random.uniform(first_key, (NX, NY, 1), jnp.float32) * jnp.log(10.0))
    entries = jax.random.truncated_normal(second_key, -6.0, 6.0, (NX, NY, NZ), jnp.float32)
    return (entries * column_scale).astype(jnp.float32)


def block_scale(own_key, extent, cuts, smallest, largest):
    def one(position, blocks):
        steps = jax.random.uniform(jax.random.fold_in(jax.random.fold_in(own_key, 6), position), (blocks,), jnp.float32, smallest / len(cuts), largest / len(cuts))
        return jnp.repeat(jnp.exp(steps), extent[position] // blocks).reshape((-1,) + (1,) * (len(extent) - position - 1))

    loudness = one(*cuts[0])
    for cut in cuts[1:]:
        loudness = loudness * one(*cut)
    return loudness


def bell_draw(key, shape, scale, reach, cuts=(), kind=jnp.bfloat16):
    values = scale * jax.random.normal(key, shape, jnp.float32)
    if cuts:
        values = values * block_scale(key, shape, cuts, -0.22, 0.18)
    return jnp.clip(values, -reach, reach).astype(kind)


def setup_inputs(seed: int = 0) -> dict:
    streams_of = jax.random.split(jax.random.key(seed), 4)
    coefficients = bell_draw(streams_of[0], (NZ, NX * NY), 1.0, 6.0, ((0, 32),))
    exponents = draw_exponents(jax.random.fold_in(streams_of[3], 71), 0)
    right_side = draw_right_side(jax.random.fold_in(streams_of[3], 71), 0)
    return dict(coefficients=coefficients, exponents=exponents, right_side=right_side)


def basis_rows():
    points = jnp.arange(4, dtype=jnp.float32)
    frequency = points[:, None]
    cosine = jnp.cos(jnp.pi * (2.0 * points[None, :] + 1.0) * frequency / 8.0)
    weight = jnp.where(frequency == 0, jnp.sqrt(jnp.float32(0.25)), jnp.sqrt(jnp.float32(0.5)))
    return (weight * cosine).astype(jnp.float32)

def reference(coefficients, exponents, right_side):
    basis = basis_rows()
    pencil_x = NX // CX
    pencil_y = NY // CY
    held = coefficients.reshape(NZ, pencil_x, pencil_y, CX, CY).transpose(1, 3, 2, 4, 0).reshape(NX, NY, NZ)
    power = exponents.reshape(BZ, pencil_x, pencil_y, CX // 4, CY // 4).transpose(1, 3, 2, 4, 0).reshape(BX, BY, BZ)
    factor = jnp.exp2(power.astype(jnp.float32))
    factor = jnp.repeat(jnp.repeat(jnp.repeat(factor, 4, axis=0), 4, axis=1), 4, axis=2)
    scaled = (held.astype(jnp.float32) * factor).astype(jnp.bfloat16)
    blocks = scaled.astype(jnp.float32).reshape(BX, 4, BY, 4, BZ, 4)
    blocks = jnp.einsum('xaybzc,ai->xiybzc', blocks, basis, precision=lax.Precision.HIGHEST)
    blocks = jnp.einsum('xiybzc,bj->xiyjzc', blocks, basis, precision=lax.Precision.HIGHEST)
    blocks = jnp.einsum('xiyjzc,ck->xiyjzk', blocks, basis, precision=lax.Precision.HIGHEST)
    decoded = blocks.reshape(NX, NY, NZ)
    padded = jnp.pad(decoded, 1)
    beside = padded[2:, 1:-1, 1:-1] + padded[:-2, 1:-1, 1:-1]
    beside = beside + padded[1:-1, 2:, 1:-1] + padded[1:-1, :-2, 1:-1]
    beside = beside + padded[1:-1, 1:-1, 2:] + padded[1:-1, 1:-1, :-2]
    residual = right_side - (6.0 * decoded - beside)
    total_sum = jnp.sum(residual * residual)
    rms = jnp.sqrt(total_sum / (NX * NY * NZ) + 1e-06)
    return (decoded, residual, rms)
```

```python
import jax
import jax.numpy as jnp
from jax import lax
from jax.sharding import PartitionSpec as P

CX = 16
CY = 24


def with_halo(cells, sides, width):
    for axis, dim in sides:
        count = lax.axis_size(axis)
        ends = count - 1
        head = lax.slice_in_dim(cells, 0, width, axis=dim)
        tail = lax.slice_in_dim(cells, cells.shape[dim] - width, cells.shape[dim], axis=dim)
        cells = jnp.concatenate(
            [
                lax.ppermute(tail, axis, [(i, (i + 1) % count) for i in range(ends)]),
                cells,
                lax.ppermute(head, axis, [((i + 1) % count, i) for i in range(ends)]),
            ],
            axis=dim,
        )
    return cells


def block_basis(width):
    rows = jnp.arange(width, dtype=jnp.int32)[:, None]
    cols = jnp.arange(width, dtype=jnp.int32)[None, :]
    frequency = (rows % 4).astype(jnp.float32)
    point = (cols % 4).astype(jnp.float32)
    weight = jnp.where(frequency == 0, jnp.sqrt(jnp.float32(0.25)), jnp.sqrt(jnp.float32(0.5)))
    entry = weight * jnp.cos(jnp.pi * (2.0 * point + 1.0) * frequency / 8.0)
    return jnp.where(rows // 4 == cols // 4, entry, 0.0)


def plane_table():
    across_x = block_basis(CX)
    across_y = block_basis(CY)
    return jnp.einsum("ux,vy->uvxy", across_x, across_y).reshape(CX * CY, CX * CY)


def spread_table():
    quarter_y = CY // 4
    blocks = jnp.arange(CX // 4 * quarter_y, dtype=jnp.int32)[:, None]
    cells = jnp.arange(CX * CY, dtype=jnp.int32)[None, :]
    same_x = cells // CY // 4 == blocks // quarter_y
    same_y = cells % CY // 4 == blocks % quarter_y
    return jnp.where(same_x & same_y, 1.0, 0.0).astype(jnp.float32)


def apply_plane(layers, table):
    return jnp.einsum(
        "zpc,cv->zpv", layers.astype(jnp.float32), table, precision=lax.Precision.HIGHEST
    )


def shards(coefficients, exponents, right_side):
    count_x = lax.axis_size("px")
    count_y = lax.axis_size("py")
    peers = count_x * count_y
    patch = CX * CY
    layer_count = coefficients.shape[0]
    block_layers = exponents.shape[0]
    table = plane_table()
    factor = jnp.exp2(exponents.astype(jnp.float32)).reshape(block_layers, peers, -1)
    spread = jnp.einsum("zpq,qc->zpc", factor, spread_table(), precision=lax.Precision.HIGHEST)
    spread = jnp.broadcast_to(spread[:, None], (block_layers, 4, peers, patch)).reshape(
        layer_count, peers, patch
    )
    scaled = (coefficients.astype(jnp.float32).reshape(layer_count, peers, patch) * spread).astype(
        jnp.bfloat16
    )
    received = lax.all_to_all(scaled, ("px", "py"), split_axis=1, concat_axis=1, tiled=True)
    arrived = apply_plane(received, table)
    stacked = arrived.transpose(1, 0, 2).reshape(-1, 128, patch)
    depth_table = block_basis(128)
    decoded = jnp.einsum(
        "nzq,zw->qnw", stacked, depth_table, precision=lax.Precision.HIGHEST
    ).reshape(CX, CY, -1)
    padded = with_halo(decoded, (("px", 0), ("py", 1)), 1)
    padded = jnp.pad(padded, ((0, 0), (0, 0), (1, 1)))
    beside = padded[2:, 1:-1, 1:-1] + padded[:-2, 1:-1, 1:-1]
    beside = beside + padded[1:-1, 2:, 1:-1] + padded[1:-1, :-2, 1:-1]
    beside = beside + padded[1:-1, 1:-1, 2:] + padded[1:-1, 1:-1, :-2]
    residual = right_side - (6.0 * decoded - beside)
    local_sum = jnp.sum(residual * residual)
    parts = lax.all_to_all(
        jnp.broadcast_to(local_sum, (peers,)), ("px", "py"), split_axis=0, concat_axis=0, tiled=True
    )
    total_sum = jnp.sum(parts)
    cell_count = decoded.shape[0] * decoded.shape[1] * decoded.shape[2] * count_x * count_y
    rms = jnp.sqrt(total_sum / cell_count + 1e-06)
    return (decoded, residual, rms)


def solution(mesh):
    return jax.shard_map(
        shards,
        mesh=mesh,
        in_specs=(P(("px", "py"), None), P(("px", "py"), None), P("px", "py", None)),
        out_specs=(P("px", "py", None), P("px", "py", None), P()),
        check_vma=False,
    )
```

```python
import functools

import jax
import jax.numpy as jnp
import numpy as np
from jax import lax
from jax.experimental import pallas as pl
from jax.experimental.pallas import tpu as pltpu
from jax.sharding import PartitionSpec as P

AXES = ("px", "py")
LANES = 128
ROWS = 56
TAIL = 48
LAYERS = 12
GROUP = 4


def basis4():
    a = np.arange(4)[:, None]
    i = np.arange(4)[None, :]
    weight = np.where(a == 0, np.sqrt(0.25), np.sqrt(0.5))
    return weight * np.cos(np.pi * (2 * i + 1) * a / 8)


def halves(table):
    table = table.astype(np.float32)
    high = table.astype(jnp.bfloat16)
    low = (table - high.astype(np.float32)).astype(jnp.bfloat16)
    return high, low


def plane(cx, cy):
    across_x = np.kron(np.eye(cx // 4), basis4())
    across_y = np.kron(np.eye(cy // 4), basis4())
    return np.kron(across_x, across_y)


def edge_table(cx, cy):
    full = plane(cx, cy).reshape(cx * cy, cx, cy)
    x_high, x_low = full[:, cx - 1, :], full[:, 0, :]
    y_high, y_low = full[:, :, cy - 1], full[:, :, 0]
    table = np.concatenate([x_high, x_low, y_high, y_low, x_high, x_low], axis=1)
    return np.concatenate(halves(table), axis=1)


def spread_table(cx, cy, per):
    quarter = cy // 4
    blocks = cx // 4 * quarter
    cell = np.arange(cx * cy)
    block = cell // cy // 4 * quarter + cell % cy // 4
    same = (np.arange(per * blocks) % blocks)[:, None] == block[None, :]
    return same.astype(jnp.bfloat16)


def depth_table():
    basis = basis4()
    table = np.zeros((5, GROUP, LAYERS, GROUP, ROWS))
    for s in range(GROUP):
        for point in range(LAYERS):
            block, k = divmod(point, 4)
            for a in range(4):
                layer = 4 * block + a
                for t in range(3):
                    table[t, s, point, s, 16 * t + layer] = basis[a, k]
                table[3, s, point, s, 16 * block + 12 + a] = basis[a, k]
                table[4, s, point, s, TAIL + a] = basis[a, k]
    return np.concatenate(halves(table.reshape(5 * GROUP * LAYERS, GROUP * ROWS)), axis=0)


def plane_windows(cx, cy):
    flipped = plane(cx, cy).T
    half = cx * cy // 2
    width = 2 * LANES
    first = flipped[:half, :width]
    second = flipped[half:, cx * cy - width :]
    return np.stack(halves(np.stack([first, second])))


def pick_table(cx, cy):
    edges = 2 * cy + 2 * cx
    table = np.zeros((edges, 2 * LANES), np.float32)
    for k in range(2 * cy):
        table[k, k] = 1
        table[k, edges + k] = 1
    for k in range(2 * cx):
        table[2 * cy + k, 2 * cy + k] = 1
        for block in range(3):
            table[2 * cy + k, LANES + 2 * cx * block + k] = 1
    return table.astype(jnp.bfloat16)


def send_kernel(
    count_x, count_y, cx, cy, coef_ref, exp_ref, spread_ref, edge_ref, out_ref, factor, scaled, edge
):
    peers = count_x * count_y
    patch = cx * cy
    blocks = patch // 16
    per = patch // blocks
    edges = 2 * cy + 2 * cx
    power = lax.shift_left(jnp.int32(1), exp_ref[...] + 15).astype(jnp.float32) * (2.0**-15)
    lane = lax.broadcasted_iota(jnp.int32, (per, patch), 1)
    row = lax.broadcasted_iota(jnp.int32, (per, patch), 0)
    own = (lane >= row * blocks) & (lane < (row + 1) * blocks)
    for h in range(peers // per):
        part = power[:, h * patch : (h + 1) * patch]
        stacked = [
            jnp.where(own, jnp.broadcast_to(part[b : b + 1], (per, patch)), 0.0) for b in range(3)
        ]
        left = jnp.concatenate(stacked, axis=0).astype(jnp.bfloat16)
        factor[h * 3 * per : (h + 1) * 3 * per, :] = jnp.dot(
            left, spread_ref[...], preferred_element_type=jnp.float32
        )
    layer = lax.broadcasted_iota(jnp.int32, (LAYERS, patch), 0)
    for p in range(peers):
        base = p // per * 3 * per + p % per
        rows = [
            jnp.broadcast_to(factor[base + b * per : base + b * per + 1, :], (LAYERS, patch))
            for b in range(3)
        ]
        spread = jnp.where(layer < 4, rows[0], jnp.where(layer < 8, rows[1], rows[2]))
        part = coef_ref[:, p * patch : (p + 1) * patch].astype(jnp.float32) * spread
        part = part.astype(jnp.bfloat16)
        scaled[p, 0:LAYERS, :] = part
        for t in range(3):
            out_ref[p, 16 * t : 16 * t + LAYERS, :] = part[:, t * LANES : (t + 1) * LANES]
    found = jnp.dot(
        scaled[...].reshape(peers * 16, patch), edge_ref[...], preferred_element_type=jnp.float32
    )
    edge[...] = (found[:, :LANES] + found[:, LANES:]).reshape(peers, 16, LANES)
    lane = lax.broadcasted_iota(jnp.int32, (16, LANES), 1)
    from_left = (lane < cy) | ((lane >= edges) & (lane < edges + cy))
    from_right = ((lane >= cy) & (lane < 2 * cy)) | (lane >= edges + cy)
    from_below = (lane >= 2 * cy) & (lane < 2 * cy + cx)
    nothing = jnp.zeros((16, LANES), jnp.float32)
    for p in range(peers):
        i, j = divmod(p, count_y)
        left = edge[p - count_y] if i > 0 else nothing
        right = edge[p + count_y] if i < count_x - 1 else nothing
        below = edge[p - 1] if j > 0 else nothing
        above = edge[p + 1] if j < count_y - 1 else nothing
        value = jnp.where(
            from_left, left, jnp.where(from_right, right, jnp.where(from_below, below, above))
        )
        high = value.astype(jnp.bfloat16).astype(jnp.float32)
        low = value - high
        tile = jnp.where(lane < edges, high, low)
        for t in range(3):
            out_ref[p, 16 * t + LAYERS : 16 * t + 16, :] = tile[4 * t : 4 * t + 4].astype(
                jnp.bfloat16
            )
        wide = lane[:4]
        first = pltpu.roll(low[0:8], LANES - 2 * cy, 1)[0:4]
        second = pltpu.roll(low[0:8], LANES - 2 * cy + 2 * cx, 1)[4:8]
        third = pltpu.roll(low[8:16], (4 * cx - 2 * cy) % LANES, 1)[0:4]
        tail = jnp.where(wide < 2 * cx, first, jnp.where(wide < 4 * cx, second, third))
        tail = jnp.where(wide < 6 * cx, tail, 0.0)
        tail = jnp.concatenate([tail, jnp.zeros((4, LANES), jnp.float32)], axis=0)
        out_ref[p, TAIL:ROWS, :] = tail.astype(jnp.bfloat16)


def split(value):
    high = value.astype(jnp.bfloat16)
    return high, (value - high.astype(jnp.float32)).astype(jnp.bfloat16)


def receive_kernel(
    cx, cy, got_ref, right_ref, depth_ref, plane_ref, pick_ref, dec_ref, res_ref, sum_ref,
    high_ref, low_ref, edge_ref,
):
    peers = got_ref.shape[0]
    depth = peers * LAYERS
    patch = cx * cy
    count = GROUP * LAYERS
    contract = (((1,), (1,)), ((), ()))
    row = lax.broadcasted_iota(jnp.int32, (count, LANES), 0)
    lane = lax.broadcasted_iota(jnp.int32, (count, LANES), 1)
    third = 2 * cx
    block = row // 4 % 3
    in_block = (lane >= block * third) & (lane < (block + 1) * third)
    for g in range(0, peers // GROUP, 2):
        messages = [
            got_ref[GROUP * h : GROUP * (h + 1)].reshape(GROUP * ROWS, LANES) for h in (g, g + 1)
        ]
        both = jnp.dot(
            depth_ref[...], jnp.concatenate(messages, axis=1), preferred_element_type=jnp.float32
        )
        both = both[: 5 * count] + both[5 * count :]
        for h in range(2):
            at = (g + h) * count
            for t in range(5):
                value = both[t * count : (t + 1) * count, h * LANES : (h + 1) * LANES]
                if t == 4:
                    value = jnp.where(in_block, value, 0.0)
                high, low = split(value)
                high_ref[at : at + count, t * LANES : (t + 1) * LANES] = high
                low_ref[at : at + count, t * LANES : (t + 1) * LANES] = low

    def across(table, ref, start):
        return lax.dot_general(
            table, ref[:, start : start + 2 * LANES], contract, preferred_element_type=jnp.float32
        )

    for w, start in enumerate((0, patch - 2 * LANES)):
        found = across(plane_ref[0, w], high_ref, start) + across(plane_ref[0, w], low_ref, start)
        found = found + across(plane_ref[1, w], high_ref, start)
        dec_ref[w * cx // 2 : (w + 1) * cx // 2] = found.reshape(cx // 2, cy, depth)
    edge_ref[...] = across(pick_ref[...], high_ref, patch) + across(pick_ref[...], low_ref, patch)

    row = lax.broadcasted_iota(jnp.int32, (cy, depth), 0)
    lane = lax.broadcasted_iota(jnp.int32, (cy, depth), 1)
    total = jnp.zeros((8, LANES), jnp.float32)
    for x in range(cx):
        here = dec_ref[x]
        beside = dec_ref[x - 1] if x > 0 else edge_ref[0:cy]
        beside = beside + (dec_ref[x + 1] if x < cx - 1 else edge_ref[cy : 2 * cy])
        low = edge_ref[2 * cy + x : 2 * cy + x + 1]
        high = edge_ref[2 * cy + cx + x : 2 * cy + cx + x + 1]
        beside = beside + jnp.where(row == 0, low, pltpu.roll(here, 1, 0))
        beside = beside + jnp.where(row == cy - 1, high, pltpu.roll(here, cy - 1, 0))
        beside = beside + jnp.where(lane == 0, 0.0, pltpu.roll(here, 1, 1))
        beside = beside + jnp.where(lane == depth - 1, 0.0, pltpu.roll(here, depth - 1, 1))
        left = right_ref[x] - (6.0 * here - beside)
        res_ref[x] = left
        square = left * left
        for r in range(0, cy, 8):
            for c in range(0, depth, LANES):
                total = total + square[r : r + 8, c : c + LANES]
    total = jnp.sum(total, axis=0, keepdims=True)
    sum_ref[...] = jnp.broadcast_to(total[None], sum_ref.shape)


def shards(count_x, count_y, coefficients, exponents, right_side):
    peers = count_x * count_y
    cx, cy, depth = right_side.shape
    patch = cx * cy
    per = 16
    vmem = pl.BlockSpec(memory_space=pltpu.VMEM)
    messages = pl.pallas_call(
        functools.partial(send_kernel, count_x, count_y, cx, cy),
        out_shape=jax.ShapeDtypeStruct((peers, ROWS, LANES), jnp.bfloat16),
        in_specs=[vmem] * 4,
        out_specs=vmem,
        scratch_shapes=[
            pltpu.VMEM((peers * 3, patch), jnp.float32),
            pltpu.VMEM((peers, 16, patch), jnp.bfloat16),
            pltpu.VMEM((peers, 16, LANES), jnp.float32),
        ],
        name="send",
    )(
        coefficients,
        exponents,
        jnp.asarray(spread_table(cx, cy, per)),
        jnp.asarray(edge_table(cx, cy)),
    )
    got = lax.all_to_all(messages, AXES, split_axis=0, concat_axis=0, tiled=True)
    decoded, residual, parts = pl.pallas_call(
        functools.partial(receive_kernel, cx, cy),
        out_shape=(
            jax.ShapeDtypeStruct((cx, cy, depth), jnp.float32),
            jax.ShapeDtypeStruct((cx, cy, depth), jnp.float32),
            jax.ShapeDtypeStruct((peers, 1, LANES), jnp.float32),
        ),
        in_specs=[vmem] * 5,
        out_specs=(vmem, vmem, vmem),
        scratch_shapes=[
            pltpu.VMEM((depth, 5 * LANES), jnp.bfloat16),
            pltpu.VMEM((depth, 5 * LANES), jnp.bfloat16),
            pltpu.VMEM((2 * cx + 2 * cy, depth), jnp.float32),
        ],
        name="receive",
    )(
        got,
        right_side,
        jnp.asarray(depth_table()),
        jnp.asarray(plane_windows(cx, cy)),
        jnp.asarray(pick_table(cx, cy)),
    )
    parts = lax.all_to_all(parts, AXES, split_axis=0, concat_axis=0, tiled=True)
    rms = jnp.sqrt(jnp.sum(parts) / (patch * depth * peers) + 1e-6)
    return (decoded, residual, rms)


def solution(mesh):
    return jax.shard_map(
        functools.partial(shards, mesh.shape["px"], mesh.shape["py"]),
        mesh=mesh,
        in_specs=(P(AXES, None), P(AXES, None), P("px", "py", None)),
        out_specs=(P("px", "py", None), P("px", "py", None), P()),
        check_vma=False,
    )
```

```python
import functools

import jax
import jax.numpy as jnp
import numpy as np
from jax import lax
from jax.experimental import pallas as pl
from jax.experimental.pallas import tpu as pltpu
from jax.sharding import PartitionSpec as P

AXES = ("px", "py")
LANES = 128
ROWS = 56
TAIL = 48
LAYERS = 12
GROUP = 4


def exchange(array):
    return lax.all_to_all(array, AXES, split_axis=0, concat_axis=0, tiled=True)


def basis4():
    a = np.arange(4)[:, None]
    i = np.arange(4)[None, :]
    weight = np.where(a == 0, np.sqrt(0.25), np.sqrt(0.5))
    return weight * np.cos(np.pi * (2 * i + 1) * a / 8)


def halves(table):
    table = table.astype(np.float32)
    high = table.astype(jnp.bfloat16)
    low = (table - high.astype(np.float32)).astype(jnp.bfloat16)
    return high, low


def plane(cx, cy):
    across_x = np.kron(np.eye(cx // 4), basis4())
    across_y = np.kron(np.eye(cy // 4), basis4())
    return np.kron(across_x, across_y)


def edge_table(cx, cy):
    full = plane(cx, cy).reshape(cx * cy, cx, cy)
    x_high, x_low = full[:, cx - 1, :], full[:, 0, :]
    y_high, y_low = full[:, :, cy - 1], full[:, :, 0]
    table = np.concatenate([x_high, x_low, y_high, y_low, x_high, x_low], axis=1)
    return np.concatenate(halves(table), axis=1)


def spread_table(cx, cy, per):
    quarter = cy // 4
    blocks = cx // 4 * quarter
    cell = np.arange(cx * cy)
    block = cell // cy // 4 * quarter + cell % cy // 4
    same = (np.arange(per * blocks) % blocks)[:, None] == block[None, :]
    return same.astype(jnp.bfloat16)


def depth_table():
    basis = basis4()
    table = np.zeros((5, GROUP, LAYERS, GROUP, ROWS))
    for s in range(GROUP):
        for point in range(LAYERS):
            block, k = divmod(point, 4)
            for a in range(4):
                layer = 4 * block + a
                for t in range(3):
                    table[t, s, point, s, 16 * t + layer] = basis[a, k]
                table[3, s, point, s, 16 * block + 12 + a] = basis[a, k]
                table[4, s, point, s, TAIL + a] = basis[a, k]
    return np.concatenate(halves(table.reshape(5 * GROUP * LAYERS, GROUP * ROWS)), axis=0)


def plane_windows(cx, cy):
    flipped = plane(cx, cy).T
    half = cx * cy // 2
    width = 2 * LANES
    first = flipped[:half, :width]
    second = flipped[half:, cx * cy - width :]
    return np.stack(halves(np.stack([first, second])))


def pick_table(cx, cy):
    edges = 2 * cy + 2 * cx
    table = np.zeros((edges, 2 * LANES), np.float32)
    for k in range(2 * cy):
        table[k, k] = 1
        table[k, edges + k] = 1
    for k in range(2 * cx):
        table[2 * cy + k, 2 * cy + k] = 1
        for block in range(3):
            table[2 * cy + k, LANES + 2 * cx * block + k] = 1
    return table.astype(jnp.bfloat16)


def send_kernel(
    count_x, count_y, cx, cy, coef_hbm, exp_hbm, spread_hbm, edge_hbm, right_hbm, table_hbm,
    out_ref, right_ref, table_ref, coef_ref, exp_ref, spread_ref, edge_ref, factor, scaled, edge, sems,
):
    pairs = [
        (exp_hbm, exp_ref), (spread_hbm, spread_ref), (coef_hbm, coef_ref), (edge_hbm, edge_ref),
        (right_hbm, right_ref), (table_hbm, table_ref),
    ]
    loads = [pltpu.make_async_copy(a, b, sems.at[n]) for n, (a, b) in enumerate(pairs)]
    for load in loads:
        load.start()
    loads[0].wait()
    loads[1].wait()
    peers = count_x * count_y
    patch = cx * cy
    blocks = patch // 16
    per = patch // blocks
    edges = 2 * cy + 2 * cx
    power = lax.shift_left(jnp.int32(1), exp_ref[...] + 15).astype(jnp.float32) * (2.0**-15)
    lane = lax.broadcasted_iota(jnp.int32, (per, patch), 1)
    row = lax.broadcasted_iota(jnp.int32, (per, patch), 0)
    own = (lane >= row * blocks) & (lane < (row + 1) * blocks)
    for h in range(peers // per):
        part = power[:, h * patch : (h + 1) * patch]
        stacked = [
            jnp.where(own, jnp.broadcast_to(part[b : b + 1], (per, patch)), 0.0) for b in range(3)
        ]
        left = jnp.concatenate(stacked, axis=0).astype(jnp.bfloat16)
        factor[h * 3 * per : (h + 1) * 3 * per, :] = jnp.dot(
            left, spread_ref[...], preferred_element_type=jnp.float32
        )
    layer = lax.broadcasted_iota(jnp.int32, (LAYERS, patch), 0)
    loads[2].wait()
    for p in range(peers):
        base = p // per * 3 * per + p % per
        rows = [
            jnp.broadcast_to(factor[base + b * per : base + b * per + 1, :], (LAYERS, patch))
            for b in range(3)
        ]
        spread = jnp.where(layer < 4, rows[0], jnp.where(layer < 8, rows[1], rows[2]))
        part = coef_ref[:, p * patch : (p + 1) * patch].astype(jnp.float32) * spread
        part = part.astype(jnp.bfloat16)
        scaled[p, 0:LAYERS, :] = part
        for t in range(3):
            out_ref[p, 16 * t : 16 * t + LAYERS, :] = part[:, t * LANES : (t + 1) * LANES]
    loads[3].wait()
    found = jnp.dot(
        scaled[...].reshape(peers * 16, patch), edge_ref[...], preferred_element_type=jnp.float32
    )
    edge[...] = (found[:, :LANES] + found[:, LANES:]).reshape(peers, 16, LANES)
    lane = lax.broadcasted_iota(jnp.int32, (16, LANES), 1)
    from_left = (lane < cy) | ((lane >= edges) & (lane < edges + cy))
    from_right = ((lane >= cy) & (lane < 2 * cy)) | (lane >= edges + cy)
    from_below = (lane >= 2 * cy) & (lane < 2 * cy + cx)
    nothing = jnp.zeros((16, LANES), jnp.float32)
    for p in range(peers):
        i, j = divmod(p, count_y)
        left = edge[p - count_y] if i > 0 else nothing
        right = edge[p + count_y] if i < count_x - 1 else nothing
        below = edge[p - 1] if j > 0 else nothing
        above = edge[p + 1] if j < count_y - 1 else nothing
        value = jnp.where(
            from_left, left, jnp.where(from_right, right, jnp.where(from_below, below, above))
        )
        high = value.astype(jnp.bfloat16).astype(jnp.float32)
        low = value - high
        tile = jnp.where(lane < edges, high, low)
        for t in range(3):
            out_ref[p, 16 * t + LAYERS : 16 * t + 16, :] = tile[4 * t : 4 * t + 4].astype(
                jnp.bfloat16
            )
        wide = lane[:4]
        first = pltpu.roll(low[0:8], LANES - 2 * cy, 1)[0:4]
        second = pltpu.roll(low[0:8], LANES - 2 * cy + 2 * cx, 1)[4:8]
        third = pltpu.roll(low[8:16], (4 * cx - 2 * cy) % LANES, 1)[0:4]
        tail = jnp.where(wide < 2 * cx, first, jnp.where(wide < 4 * cx, second, third))
        tail = jnp.where(wide < 6 * cx, tail, 0.0)
        tail = jnp.concatenate([tail, jnp.zeros((4, LANES), jnp.float32)], axis=0)
        out_ref[p, TAIL:ROWS, :] = tail.astype(jnp.bfloat16)
    loads[4].wait()
    loads[5].wait()


def receive_table(cx, cy):
    depth = depth_table()
    depth = np.pad(depth, ((0, 0), (0, 2 * LANES - depth.shape[1])))
    planes = plane_windows(cx, cy).reshape(-1, 2 * LANES)
    return np.concatenate([depth, planes, pick_table(cx, cy)], axis=0)


def split(value):
    high = value.astype(jnp.bfloat16)
    return high, (value - high.astype(jnp.float32)).astype(jnp.bfloat16)


def receive_kernel(
    cx, cy, got_ref, right_ref, table_ref, dec_hbm, res_hbm, sum_ref,
    high_ref, low_ref, edge_ref, dec_ref, res_ref, sems,
):
    peers = got_ref.shape[0]
    depth = peers * LAYERS
    patch = cx * cy
    count = GROUP * LAYERS
    contract = (((1,), (1,)), ((), ()))
    row = lax.broadcasted_iota(jnp.int32, (count, LANES), 0)
    lane = lax.broadcasted_iota(jnp.int32, (count, LANES), 1)
    third = 2 * cx
    half = patch // 2
    tables = 10 * count
    flat = [table_ref[tables + half * n : tables + half * (n + 1)] for n in range(4)]
    pick = table_ref[tables + 4 * half :]
    block = row // 4 % 3
    in_block = (lane >= block * third) & (lane < (block + 1) * third)
    for g in range(0, peers // GROUP, 2):
        messages = [
            got_ref[GROUP * h : GROUP * (h + 1)].reshape(GROUP * ROWS, LANES) for h in (g, g + 1)
        ]
        both = jnp.dot(
            table_ref[:tables, : GROUP * ROWS], jnp.concatenate(messages, axis=1), preferred_element_type=jnp.float32
        )
        both = both[: 5 * count] + both[5 * count :]
        for h in range(2):
            at = (g + h) * count
            for t in range(5):
                value = both[t * count : (t + 1) * count, h * LANES : (h + 1) * LANES]
                if t == 4:
                    value = jnp.where(in_block, value, 0.0)
                high, low = split(value)
                high_ref[at : at + count, t * LANES : (t + 1) * LANES] = high
                low_ref[at : at + count, t * LANES : (t + 1) * LANES] = low

    def across(table, ref, start):
        return lax.dot_general(
            table, ref[:, start : start + 2 * LANES], contract, preferred_element_type=jnp.float32
        )

    stores = []
    for w, start in enumerate((0, patch - 2 * LANES)):
        found = across(flat[w], high_ref, start) + across(flat[w], low_ref, start)
        found = found + across(flat[2 + w], high_ref, start)
        part = pl.ds(w * cx // 2, cx // 2)
        dec_ref[part] = found.reshape(cx // 2, cy, depth)
        stores.append(pltpu.make_async_copy(dec_ref.at[part], dec_hbm.at[part], sems.at[w]))
        stores[-1].start()
    edge_ref[...] = across(pick, high_ref, patch) + across(pick, low_ref, patch)

    row = lax.broadcasted_iota(jnp.int32, (cy, depth), 0)
    lane = lax.broadcasted_iota(jnp.int32, (cy, depth), 1)
    total = jnp.zeros((8, LANES), jnp.float32)
    for x in range(cx):
        here = dec_ref[x]
        beside = dec_ref[x - 1] if x > 0 else edge_ref[0:cy]
        beside = beside + (dec_ref[x + 1] if x < cx - 1 else edge_ref[cy : 2 * cy])
        low = edge_ref[2 * cy + x : 2 * cy + x + 1]
        high = edge_ref[2 * cy + cx + x : 2 * cy + cx + x + 1]
        beside = beside + jnp.where(row == 0, low, pltpu.roll(here, 1, 0))
        beside = beside + jnp.where(row == cy - 1, high, pltpu.roll(here, cy - 1, 0))
        beside = beside + jnp.where(lane == 0, 0.0, pltpu.roll(here, 1, 1))
        beside = beside + jnp.where(lane == depth - 1, 0.0, pltpu.roll(here, depth - 1, 1))
        left = right_ref[x] - (6.0 * here - beside)
        res_ref[x] = left
        square = left * left
        for r in range(0, cy, 8):
            for c in range(0, depth, LANES):
                total = total + square[r : r + 8, c : c + LANES]
        if x % 4 == 3:
            part = pl.ds(x - 3, 4)
            stores.append(
                pltpu.make_async_copy(res_ref.at[part], res_hbm.at[part], sems.at[2 + x // 4])
            )
            stores[-1].start()
    total = jnp.sum(total, axis=0, keepdims=True)
    sum_ref[...] = jnp.broadcast_to(total[None], sum_ref.shape)
    for store in stores:
        store.wait()


def finish_kernel(cells, parts_ref, rms_ref):
    total = jnp.sum(parts_ref[...].reshape(-1, LANES), axis=0, keepdims=True)
    total = jnp.sum(total, axis=1, keepdims=True)
    rms_ref[...] = jnp.sqrt(total / cells + 1e-6)


def shards(count_x, count_y, coefficients, exponents, right_side):
    peers = count_x * count_y
    cx, cy, depth = right_side.shape
    patch = cx * cy
    per = 16
    vmem = pl.BlockSpec(memory_space=pltpu.VMEM)
    hbm = pl.BlockSpec(memory_space=pltpu.HBM)
    tables = jnp.asarray(receive_table(cx, cy))
    kept = [(right_side.shape, right_side.dtype), (tables.shape, tables.dtype)]
    kept = [((peers, ROWS, LANES), jnp.bfloat16)] + kept
    held = sum(int(np.prod(shape)) * jnp.dtype(dtype).itemsize for shape, dtype in kept)
    near = held <= 2 << 20
    place = pltpu.VMEM if near else jax.ShapeDtypeStruct
    messages, right_side, tables = pl.pallas_call(
        functools.partial(send_kernel, count_x, count_y, cx, cy),
        out_shape=[place(*k) for k in kept],
        in_specs=[hbm] * 6,
        out_specs=[vmem] * 3,
        scratch_shapes=[
            pltpu.VMEM(coefficients.shape, coefficients.dtype),
            pltpu.VMEM(exponents.shape, exponents.dtype),
            pltpu.VMEM((patch, patch), jnp.bfloat16),
            pltpu.VMEM((patch, 2 * LANES), jnp.bfloat16),
            pltpu.VMEM((peers * 3, patch), jnp.float32),
            pltpu.VMEM((peers, 16, patch), jnp.bfloat16),
            pltpu.VMEM((peers, 16, LANES), jnp.float32),
            pltpu.SemaphoreType.DMA((6,)),
        ],
        compiler_params=pltpu.CompilerParams(
            vmem_limit_bytes=(64 << 20) - held - (256 << 10) if near else 48 << 20
        ),
        name="send",
    )(
        coefficients,
        exponents,
        jnp.asarray(spread_table(cx, cy, per)),
        jnp.asarray(edge_table(cx, cy)),
        right_side,
        tables,
    )
    got = exchange(messages)
    decoded, residual, parts = pl.pallas_call(
        functools.partial(receive_kernel, cx, cy),
        out_shape=(
            jax.ShapeDtypeStruct((cx, cy, depth), jnp.float32),
            jax.ShapeDtypeStruct((cx, cy, depth), jnp.float32),
            pltpu.VMEM((peers, 1, LANES), jnp.float32),
        ),
        in_specs=[vmem] * 3,
        out_specs=(hbm, hbm, vmem),
        scratch_shapes=[
            pltpu.VMEM((depth, 5 * LANES), jnp.bfloat16),
            pltpu.VMEM((depth, 5 * LANES), jnp.bfloat16),
            pltpu.VMEM((2 * cx + 2 * cy, depth), jnp.float32),
            pltpu.VMEM((cx, cy, depth), jnp.float32),
            pltpu.VMEM((cx, cy, depth), jnp.float32),
            pltpu.SemaphoreType.DMA((2 + cx // 4,)),
        ],
        compiler_params=pltpu.CompilerParams(vmem_limit_bytes=(12 << 20) * peers // 32),
        name="receive",
    )(got, right_side, tables)
    parts = exchange(parts)
    rms = pl.pallas_call(
        functools.partial(finish_kernel, patch * depth * peers),
        out_shape=jax.ShapeDtypeStruct((1, 1), jnp.float32),
        in_specs=[vmem],
        out_specs=vmem,
        compiler_params=pltpu.CompilerParams(vmem_limit_bytes=1 << 20),
        name="finish",
    )(parts)
    return (decoded, residual, rms.reshape(()))


def solution(mesh):
    return jax.shard_map(
        functools.partial(shards, mesh.shape["px"], mesh.shape["py"]),
        mesh=mesh,
        in_specs=(P(AXES, None), P(AXES, None), P("px", "py", None)),
        out_specs=(P("px", "py", None), P("px", "py", None), P()),
        check_vma=False,
    )
```

```python
import functools

import jax
import jax.numpy as jnp
import numpy as np
from jax import lax
from jax.experimental import pallas as pl
from jax.experimental.pallas import tpu as pltpu
from jax.sharding import PartitionSpec as P

AXES = ("px", "py")
LANES = 128
ROWS = 52
TAIL = 48
LAYERS = 12
GROUP = 4


def exchange(array):
    return lax.all_to_all(array, AXES, split_axis=0, concat_axis=0, tiled=True)


def basis4():
    a = np.arange(4)[:, None]
    i = np.arange(4)[None, :]
    weight = np.where(a == 0, np.sqrt(0.25), np.sqrt(0.5))
    return weight * np.cos(np.pi * (2 * i + 1) * a / 8)


def halves(table):
    table = table.astype(np.float32)
    high = table.astype(jnp.bfloat16)
    low = (table - high.astype(np.float32)).astype(jnp.bfloat16)
    return high, low


def plane(cx, cy):
    across_x = np.kron(np.eye(cx // 4), basis4())
    across_y = np.kron(np.eye(cy // 4), basis4())
    return np.kron(across_x, across_y)


def edge_table(cx, cy):
    full = plane(cx, cy).reshape(cx * cy, cx, cy)
    x_high, x_low = full[:, cx - 1, :], full[:, 0, :]
    y_high, y_low = full[:, :, cy - 1], full[:, :, 0]
    table = np.concatenate([x_high, x_low, y_high, y_low, x_high, x_low], axis=1)
    return np.concatenate(halves(table), axis=1)


def depth_table():
    basis = basis4()
    table = np.zeros((5, GROUP, LAYERS, GROUP, ROWS))
    for s in range(GROUP):
        for point in range(LAYERS):
            block, k = divmod(point, 4)
            for a in range(4):
                layer = 4 * block + a
                for t in range(3):
                    table[t, s, point, s, 16 * t + layer] = basis[a, k]
                table[3, s, point, s, 16 * block + 12 + a] = basis[a, k]
                table[4, s, point, s, TAIL + a] = basis[a, k]
    return np.concatenate(halves(table.reshape(5 * GROUP * LAYERS, GROUP * ROWS)), axis=0)


def plane_windows(cx, cy):
    flipped = plane(cx, cy).T
    half = cx * cy // 2
    width = 2 * LANES
    first = flipped[:half, :width]
    second = flipped[half:, cx * cy - width :]
    return np.stack(halves(np.stack([first, second])))


def pick_table(cx, cy):
    edges = 2 * cy + 2 * cx
    table = np.zeros((edges, 2 * LANES), np.float32)
    for k in range(2 * cy):
        table[k, k] = 1
        table[k, edges + k] = 1
    for k in range(2 * cx):
        table[2 * cy + k, 2 * cy + k] = 1
        for block in range(3):
            table[2 * cy + k, LANES + 2 * cx * block + k] = 1
    return table.astype(jnp.bfloat16)


def spread_table(cx, cy):
    blocks, patch = cx * cy // 16, cx * cy
    own = lax.broadcasted_iota(jnp.int32, (patch, patch), 0) % blocks
    cell = lax.broadcasted_iota(jnp.int32, (1, patch), 1)
    block = cell // (4 * cy) * (cy // 4) + cell % cy // 4
    return jnp.where(own == block, 1.0, 0.0).astype(jnp.bfloat16)


def send_kernel(
    count_x, count_y, cx, cy, coef_hbm, exp_hbm, edge_hbm, right_hbm, table_hbm,
    out_ref, right_ref, table_ref, coef_ref, exp_ref, edge_ref, factor, scaled, edge, sems,
):
    pairs = [(exp_hbm, exp_ref), (coef_hbm, coef_ref), (edge_hbm, edge_ref)]
    pairs += [(right_hbm, right_ref), (table_hbm, table_ref)]
    loads = [pltpu.make_async_copy(a, b, sems.at[n]) for n, (a, b) in enumerate(pairs)]
    for load in loads:
        load.start()
    peers = count_x * count_y
    patch = cx * cy
    blocks = patch // 16
    per = patch // blocks
    edges = 2 * cy + 2 * cx
    spread = spread_table(cx, cy)
    loads[0].wait()
    power = lax.shift_left(jnp.int32(1), exp_ref[...] + 15).astype(jnp.float32) * (2.0**-15)
    lane = lax.broadcasted_iota(jnp.int32, (per, patch), 1)
    row = lax.broadcasted_iota(jnp.int32, (per, patch), 0)
    own = (lane >= row * blocks) & (lane < (row + 1) * blocks)
    for h in range(peers // per):
        part = power[:, h * patch : (h + 1) * patch]
        stacked = [
            jnp.where(own, jnp.broadcast_to(part[b : b + 1], (per, patch)), 0.0) for b in range(3)
        ]
        left = jnp.concatenate(stacked, axis=0).astype(jnp.bfloat16)
        factor[h * 3 * per : (h + 1) * 3 * per, :] = jnp.dot(
            left, spread, preferred_element_type=jnp.float32
        )
    layer = lax.broadcasted_iota(jnp.int32, (LAYERS, patch), 0)
    wide = lax.broadcasted_iota(jnp.int32, (4, LANES), 1)
    lane = lax.broadcasted_iota(jnp.int32, (16, LANES), 1)
    from_left = (lane < cy) | ((lane >= edges) & (lane < edges + cy))
    from_right = ((lane >= cy) & (lane < 2 * cy)) | (lane >= edges + cy)
    from_below = (lane >= 2 * cy) & (lane < 2 * cy + cx)
    nothing = jnp.zeros((16, LANES), jnp.float32)

    def scale_row(i):
        for p in range(i * count_y, (i + 1) * count_y):
            base = p // per * 3 * per + p % per
            rows = [
                jnp.broadcast_to(factor[base + b * per : base + b * per + 1, :], (LAYERS, patch))
                for b in range(3)
            ]
            scale = jnp.where(layer < 4, rows[0], jnp.where(layer < 8, rows[1], rows[2]))
            part = coef_ref[:, p * patch : (p + 1) * patch].astype(jnp.float32) * scale
            part = part.astype(jnp.bfloat16)
            scaled[p, 0:LAYERS, :] = part
            for t in range(3):
                tile = part[:, t * LANES : (t + 1) * LANES]
                for k in range(3):
                    out_ref[p, 4 * t + k] = tile[4 * k : 4 * k + 4]
        row = pl.ds(i * count_y, count_y)
        found = jnp.dot(
            scaled[row].reshape(count_y * 16, patch),
            edge_ref[...],
            preferred_element_type=jnp.float32,
        )
        edge[row] = (found[:, :LANES] + found[:, LANES:]).reshape(count_y, 16, LANES)

    def join_row(i):
        for p in range(i * count_y, (i + 1) * count_y):
            j = p % count_y
            left = edge[p - count_y] if i > 0 else nothing
            right = edge[p + count_y] if i < count_x - 1 else nothing
            below = edge[p - 1] if j > 0 else nothing
            above = edge[p + 1] if j < count_y - 1 else nothing
            value = jnp.where(
                from_left, left, jnp.where(from_right, right, jnp.where(from_below, below, above))
            )
            high = value.astype(jnp.bfloat16).astype(jnp.float32)
            low = value - high
            tile = jnp.where(lane < edges, high, low).astype(jnp.bfloat16)
            for t in range(3):
                out_ref[p, 4 * t + 3] = tile[4 * t : 4 * t + 4]
            first = pltpu.roll(low[0:8], LANES - 2 * cy, 1)[0:4]
            second = pltpu.roll(low[0:8], LANES - 2 * cy + 2 * cx, 1)[4:8]
            third = pltpu.roll(low[8:16], (4 * cx - 2 * cy) % LANES, 1)[0:4]
            tail = jnp.where(wide < 2 * cx, first, jnp.where(wide < 4 * cx, second, third))
            tail = jnp.where(wide < 6 * cx, tail, 0.0)
            out_ref[p, TAIL // 4] = tail.astype(jnp.bfloat16)

    loads[1].wait()
    loads[2].wait()
    for i in range(count_x):
        scale_row(i)
        if i > 0:
            join_row(i - 1)
    join_row(count_x - 1)
    loads[3].wait()
    loads[4].wait()


def receive_table(cx, cy):
    depth = depth_table()
    depth = np.pad(depth, ((0, 0), (0, 2 * LANES - depth.shape[1])))
    planes = plane_windows(cx, cy).reshape(-1, 2 * LANES)
    return np.concatenate([depth, planes, pick_table(cx, cy)], axis=0)


def split(value):
    high = value.astype(jnp.bfloat16)
    return high, (value - high.astype(jnp.float32)).astype(jnp.bfloat16)


def receive_kernel(
    cx, cy, got_ref, right_ref, table_ref, dec_hbm, res_hbm, sum_ref,
    high_ref, low_ref, edge_ref, dec_ref, res_ref, sems,
):
    peers = got_ref.shape[0]
    depth = peers * LAYERS
    patch = cx * cy
    count = GROUP * LAYERS
    contract = (((1,), (1,)), ((), ()))
    row = lax.broadcasted_iota(jnp.int32, (count, LANES), 0)
    lane = lax.broadcasted_iota(jnp.int32, (count, LANES), 1)
    third = 2 * cx
    half = patch // 2
    tables = 10 * count
    flat = [table_ref[tables + half * n : tables + half * (n + 1)] for n in range(4)]
    pick = table_ref[tables + 4 * half :]
    block = row // 4 % 3
    in_block = (lane >= block * third) & (lane < (block + 1) * third)
    for g in range(0, peers // GROUP, 2):
        messages = [
            got_ref[GROUP * h : GROUP * (h + 1)].reshape(GROUP * ROWS, LANES) for h in (g, g + 1)
        ]
        both = jnp.dot(
            table_ref[:tables, : GROUP * ROWS], jnp.concatenate(messages, axis=1), preferred_element_type=jnp.float32
        )
        both = both[: 5 * count] + both[5 * count :]
        for h in range(2):
            at = (g + h) * count
            for t in range(5):
                value = both[t * count : (t + 1) * count, h * LANES : (h + 1) * LANES]
                if t == 4:
                    value = jnp.where(in_block, value, 0.0)
                high, low = split(value)
                high_ref[at : at + count, t * LANES : (t + 1) * LANES] = high
                low_ref[at : at + count, t * LANES : (t + 1) * LANES] = low

    def across(table, ref, start):
        return lax.dot_general(
            table, ref[:, start : start + 2 * LANES], contract, preferred_element_type=jnp.float32
        )

    stores = []
    for w, start in enumerate((0, patch - 2 * LANES)):
        found = across(flat[w], high_ref, start) + across(flat[w], low_ref, start)
        found = found + across(flat[2 + w], high_ref, start)
        part = pl.ds(w * cx // 2, cx // 2)
        dec_ref[part] = found.reshape(cx // 2, cy, depth)
        stores.append(pltpu.make_async_copy(dec_ref.at[part], dec_hbm.at[part], sems.at[w]))
        stores[-1].start()
    edge_ref[...] = across(pick, high_ref, patch) + across(pick, low_ref, patch)

    row = lax.broadcasted_iota(jnp.int32, (cy, depth), 0)
    lane = lax.broadcasted_iota(jnp.int32, (cy, depth), 1)
    total = jnp.zeros((8, LANES), jnp.float32)
    for x in range(cx):
        here = dec_ref[x]
        beside = dec_ref[x - 1] if x > 0 else edge_ref[0:cy]
        beside = beside + (dec_ref[x + 1] if x < cx - 1 else edge_ref[cy : 2 * cy])
        low = edge_ref[2 * cy + x : 2 * cy + x + 1]
        high = edge_ref[2 * cy + cx + x : 2 * cy + cx + x + 1]
        beside = beside + jnp.where(row == 0, low, pltpu.roll(here, 1, 0))
        beside = beside + jnp.where(row == cy - 1, high, pltpu.roll(here, cy - 1, 0))
        beside = beside + jnp.where(lane == 0, 0.0, pltpu.roll(here, 1, 1))
        beside = beside + jnp.where(lane == depth - 1, 0.0, pltpu.roll(here, depth - 1, 1))
        left = right_ref[x] - (6.0 * here - beside)
        res_ref[x] = left
        square = left * left
        for r in range(0, cy, 8):
            for c in range(0, depth, LANES):
                total = total + square[r : r + 8, c : c + LANES]
        if x % 4 == 3:
            part = pl.ds(x - 3, 4)
            stores.append(
                pltpu.make_async_copy(res_ref.at[part], res_hbm.at[part], sems.at[2 + x // 4])
            )
            stores[-1].start()
    total = jnp.sum(total, axis=0, keepdims=True)
    sum_ref[...] = jnp.broadcast_to(total[None], sum_ref.shape)
    for store in stores:
        store.wait()


def finish_kernel(cells, parts_ref, rms_ref):
    total = jnp.sum(parts_ref[...].reshape(-1, LANES), axis=0, keepdims=True)
    total = jnp.sum(total, axis=1, keepdims=True)
    rms_ref[...] = jnp.sqrt(total / cells + 1e-6)


def shards(count_x, count_y, coefficients, exponents, right_side):
    peers = count_x * count_y
    cx, cy, depth = right_side.shape
    patch = cx * cy
    vmem = pl.BlockSpec(memory_space=pltpu.VMEM)
    hbm = pl.BlockSpec(memory_space=pltpu.HBM)
    tables = jnp.asarray(receive_table(cx, cy))
    kept = [(right_side.shape, right_side.dtype), (tables.shape, tables.dtype)]
    kept = [((peers, ROWS // 4, 4, LANES), jnp.bfloat16)] + kept
    held = sum(int(np.prod(shape)) * jnp.dtype(dtype).itemsize for shape, dtype in kept)
    near = held <= 2 << 20
    place = pltpu.VMEM if near else jax.ShapeDtypeStruct
    messages, right_side, tables = pl.pallas_call(
        functools.partial(send_kernel, count_x, count_y, cx, cy),
        out_shape=[place(*k) for k in kept],
        in_specs=[hbm] * 5,
        out_specs=[vmem] * 3,
        scratch_shapes=[
            pltpu.VMEM(coefficients.shape, coefficients.dtype),
            pltpu.VMEM(exponents.shape, exponents.dtype),
            pltpu.VMEM((patch, 2 * LANES), jnp.bfloat16),
            pltpu.VMEM((peers * 3, patch), jnp.float32),
            pltpu.VMEM((peers, 16, patch), jnp.bfloat16),
            pltpu.VMEM((peers, 16, LANES), jnp.float32),
            pltpu.SemaphoreType.DMA((5,)),
        ],
        compiler_params=pltpu.CompilerParams(
            vmem_limit_bytes=(64 << 20) - held - (256 << 10) if near else 48 << 20
        ),
        name="send",
    )(
        coefficients,
        exponents,
        jnp.asarray(edge_table(cx, cy)),
        right_side,
        tables,
    )
    got = exchange(messages)
    decoded, residual, parts = pl.pallas_call(
        functools.partial(receive_kernel, cx, cy),
        out_shape=(
            jax.ShapeDtypeStruct((cx, cy, depth), jnp.float32),
            jax.ShapeDtypeStruct((cx, cy, depth), jnp.float32),
            pltpu.VMEM((peers, 1, LANES), jnp.float32),
        ),
        in_specs=[vmem] * 3,
        out_specs=(hbm, hbm, vmem),
        scratch_shapes=[
            pltpu.VMEM((depth, 5 * LANES), jnp.bfloat16),
            pltpu.VMEM((depth, 5 * LANES), jnp.bfloat16),
            pltpu.VMEM((2 * cx + 2 * cy, depth), jnp.float32),
            pltpu.VMEM((cx, cy, depth), jnp.float32),
            pltpu.VMEM((cx, cy, depth), jnp.float32),
            pltpu.SemaphoreType.DMA((2 + cx // 4,)),
        ],
        compiler_params=pltpu.CompilerParams(vmem_limit_bytes=(12 << 20) * peers // 32),
        name="receive",
    )(got, right_side, tables)
    parts = exchange(parts)
    rms = pl.pallas_call(
        functools.partial(finish_kernel, patch * depth * peers),
        out_shape=jax.ShapeDtypeStruct((1, 1), jnp.float32),
        in_specs=[vmem],
        out_specs=vmem,
        compiler_params=pltpu.CompilerParams(vmem_limit_bytes=1 << 20),
        name="finish",
    )(parts)
    return (decoded, residual, rms.reshape(()))


def solution(mesh):
    return jax.shard_map(
        functools.partial(shards, mesh.shape["px"], mesh.shape["py"]),
        mesh=mesh,
        in_specs=(P(AXES, None), P(AXES, None), P("px", "py", None)),
        out_specs=(P("px", "py", None), P("px", "py", None), P()),
        check_vma=False,
    )
```

```python
import functools

import jax
import jax.numpy as jnp
import numpy as np
from jax import lax
from jax.experimental import pallas as pl
from jax.experimental.pallas import tpu as pltpu
from jax.sharding import PartitionSpec as P

AXES = ("px", "py")
LANES = 128
ROWS = 52
TAIL = 48
LAYERS = 12
GROUP = 4
SEQUENCE = (7, 4, 3, 2, 5, 6, 1, 0)
WITHIN = (1, 3, 0, 2)


def order_of(count_x, count_y):
    groups = count_x * count_y // GROUP
    order = SEQUENCE if groups == len(SEQUENCE) else range(groups)
    return [GROUP * g + d for g in order for d in WITHIN]


def exchange(array, order):
    return lax.all_to_all(
        array, AXES, split_axis=0, concat_axis=0, tiled=True, axis_index_groups=[order]
    )


def basis4():
    a = np.arange(4)[:, None]
    i = np.arange(4)[None, :]
    weight = np.where(a == 0, np.sqrt(0.25), np.sqrt(0.5))
    return weight * np.cos(np.pi * (2 * i + 1) * a / 8)


def halves(table):
    table = table.astype(np.float32)
    high = table.astype(jnp.bfloat16)
    low = (table - high.astype(np.float32)).astype(jnp.bfloat16)
    return high, low


def plane(cx, cy):
    across_x = np.kron(np.eye(cx // 4), basis4())
    across_y = np.kron(np.eye(cy // 4), basis4())
    return np.kron(across_x, across_y)


def edge_table(cx, cy):
    full = plane(cx, cy).reshape(cx * cy, cx, cy)
    x_high, x_low = full[:, cx - 1, :], full[:, 0, :]
    y_high, y_low = full[:, :, cy - 1], full[:, :, 0]
    table = np.concatenate([x_high, x_low, y_high, y_low, x_high, x_low], axis=1)
    return np.concatenate(halves(table), axis=1)


def depth_table(order):
    at = np.argsort([d % GROUP for d in order[:GROUP]])
    basis = basis4()
    table = np.zeros((5, GROUP, LAYERS, GROUP, ROWS))
    for s in range(GROUP):
        for point in range(LAYERS):
            block, k = divmod(point, 4)
            for a in range(4):
                layer = 4 * block + a
                for t in range(3):
                    table[t, s, point, at[s], 16 * t + layer] = basis[a, k]
                table[3, s, point, at[s], 16 * block + 12 + a] = basis[a, k]
                table[4, s, point, at[s], TAIL + a] = basis[a, k]
    return np.concatenate(halves(table.reshape(5 * GROUP * LAYERS, GROUP * ROWS)), axis=0)


def plane_windows(cx, cy):
    flipped = plane(cx, cy).T
    half = cx * cy // 2
    width = 2 * LANES
    first = flipped[:half, :width]
    second = flipped[half:, cx * cy - width :]
    return np.stack(halves(np.stack([first, second])))


def pick_table(cx, cy):
    edges = 2 * cy + 2 * cx
    table = np.zeros((edges, 2 * LANES), np.float32)
    for k in range(2 * cy):
        table[k, k] = 1
        table[k, edges + k] = 1
    for k in range(2 * cx):
        table[2 * cy + k, 2 * cy + k] = 1
        for block in range(3):
            table[2 * cy + k, LANES + 2 * cx * block + k] = 1
    return table.astype(jnp.bfloat16)


def spread_table(cx, cy):
    blocks, patch = cx * cy // 16, cx * cy
    own = lax.broadcasted_iota(jnp.int32, (patch, patch), 0) % blocks
    cell = lax.broadcasted_iota(jnp.int32, (1, patch), 1)
    block = cell // (4 * cy) * (cy // 4) + cell % cy // 4
    return jnp.where(own == block, 1.0, 0.0).astype(jnp.bfloat16)


def send_kernel(
    order, count_x, count_y, cx, cy, coef_hbm, exp_hbm, edge_hbm, right_hbm, table_hbm,
    out_ref, right_ref, table_ref, coef_ref, exp_ref, edge_ref, factor, scaled, edge, sems,
):
    pairs = [(exp_hbm, exp_ref), (coef_hbm, coef_ref), (edge_hbm, edge_ref)]
    pairs += [(right_hbm, right_ref), (table_hbm, table_ref)]
    loads = [pltpu.make_async_copy(a, b, sems.at[n]) for n, (a, b) in enumerate(pairs)]
    for load in loads:
        load.start()
    peers = count_x * count_y
    place = np.argsort(order)
    patch = cx * cy
    blocks = patch // 16
    per = patch // blocks
    edges = 2 * cy + 2 * cx
    spread = spread_table(cx, cy)
    loads[0].wait()
    power = lax.shift_left(jnp.int32(1), exp_ref[...] + 15).astype(jnp.float32) * (2.0**-15)
    lane = lax.broadcasted_iota(jnp.int32, (per, patch), 1)
    row = lax.broadcasted_iota(jnp.int32, (per, patch), 0)
    own = (lane >= row * blocks) & (lane < (row + 1) * blocks)
    for h in range(peers // per):
        part = power[:, h * patch : (h + 1) * patch]
        stacked = [
            jnp.where(own, jnp.broadcast_to(part[b : b + 1], (per, patch)), 0.0) for b in range(3)
        ]
        left = jnp.concatenate(stacked, axis=0).astype(jnp.bfloat16)
        factor[h * 3 * per : (h + 1) * 3 * per, :] = jnp.dot(
            left, spread, preferred_element_type=jnp.float32
        )
    layer = lax.broadcasted_iota(jnp.int32, (LAYERS, patch), 0)
    wide = lax.broadcasted_iota(jnp.int32, (4, LANES), 1)
    lane = lax.broadcasted_iota(jnp.int32, (16, LANES), 1)
    from_left = (lane < cy) | ((lane >= edges) & (lane < edges + cy))
    from_right = ((lane >= cy) & (lane < 2 * cy)) | (lane >= edges + cy)
    from_below = (lane >= 2 * cy) & (lane < 2 * cy + cx)
    nothing = jnp.zeros((16, LANES), jnp.float32)

    for p in range(peers):
        base = p // per * 3 * per + p % per
        rows = [
            jnp.broadcast_to(factor[base + b * per : base + b * per + 1, :], (LAYERS, patch))
            for b in range(3)
        ]
        scale = jnp.where(layer < 4, rows[0], jnp.where(layer < 8, rows[1], rows[2]))
        scaled[p, 0:LAYERS, :] = scale.astype(jnp.bfloat16)

    def scale_row(i):
        for p in range(i * count_y, (i + 1) * count_y):
            part = coef_ref[:, p * patch : (p + 1) * patch] * scaled[p, 0:LAYERS, :]
            scaled[p, 0:LAYERS, :] = part
            for t in range(3):
                tile = part[:, t * LANES : (t + 1) * LANES]
                for k in range(3):
                    out_ref[place[p], 4 * t + k] = tile[4 * k : 4 * k + 4]
        row = pl.ds(i * count_y, count_y)
        found = jnp.dot(
            scaled[row].reshape(count_y * 16, patch),
            edge_ref[...],
            preferred_element_type=jnp.float32,
        )
        edge[row] = (found[:, :LANES] + found[:, LANES:]).reshape(count_y, 16, LANES)

    def join_row(i):
        for p in range(i * count_y, (i + 1) * count_y):
            j = p % count_y
            left = edge[p - count_y] if i > 0 else nothing
            right = edge[p + count_y] if i < count_x - 1 else nothing
            below = edge[p - 1] if j > 0 else nothing
            above = edge[p + 1] if j < count_y - 1 else nothing
            value = jnp.where(
                from_left, left, jnp.where(from_right, right, jnp.where(from_below, below, above))
            )
            high = value.astype(jnp.bfloat16).astype(jnp.float32)
            low = value - high
            tile = jnp.where(lane < edges, high, low).astype(jnp.bfloat16)
            for t in range(3):
                out_ref[place[p], 4 * t + 3] = tile[4 * t : 4 * t + 4]
            first = pltpu.roll(low[0:8], LANES - 2 * cy, 1)[0:4]
            second = pltpu.roll(low[0:8], LANES - 2 * cy + 2 * cx, 1)[4:8]
            third = pltpu.roll(low[8:16], (4 * cx - 2 * cy) % LANES, 1)[0:4]
            tail = jnp.where(wide < 2 * cx, first, jnp.where(wide < 4 * cx, second, third))
            tail = jnp.where(wide < 6 * cx, tail, 0.0)
            out_ref[place[p], TAIL // 4] = tail.astype(jnp.bfloat16)

    loads[1].wait()
    loads[2].wait()
    for i in range(count_x):
        scale_row(i)
        if i > 0:
            join_row(i - 1)
    join_row(count_x - 1)
    loads[3].wait()
    loads[4].wait()


def receive_table(order, cx, cy):
    depth = depth_table(order)
    depth = np.pad(depth, ((0, 0), (0, 2 * LANES - depth.shape[1])))
    planes = plane_windows(cx, cy).reshape(-1, 2 * LANES)
    return np.concatenate([depth, planes, pick_table(cx, cy)], axis=0)


def split(value):
    high = value.astype(jnp.bfloat16)
    return high, (value - high.astype(jnp.float32)).astype(jnp.bfloat16)


def receive_kernel(
    order, cx, cy, got_ref, right_ref, table_ref, dec_hbm, res_hbm, sum_ref,
    high_ref, low_ref, edge_ref, dec_ref, res_ref, sems,
):
    peers = got_ref.shape[0]
    groups = np.argsort([d // GROUP for d in order[::GROUP]])
    depth = peers * LAYERS
    patch = cx * cy
    count = GROUP * LAYERS
    contract = (((1,), (1,)), ((), ()))
    row = lax.broadcasted_iota(jnp.int32, (count, LANES), 0)
    lane = lax.broadcasted_iota(jnp.int32, (count, LANES), 1)
    third = 2 * cx
    half = patch // 2
    tables = 10 * count
    flat = [table_ref[tables + half * n : tables + half * (n + 1)] for n in range(4)]
    pick = table_ref[tables + 4 * half :]
    block = row // 4 % 3
    in_block = (lane >= block * third) & (lane < (block + 1) * third)
    for g in range(0, peers // GROUP, 2):
        messages = [
            got_ref[GROUP * h : GROUP * (h + 1)].reshape(GROUP * ROWS, LANES)
            for h in (groups[g], groups[g + 1])
        ]
        both = jnp.dot(
            table_ref[:tables, : GROUP * ROWS], jnp.concatenate(messages, axis=1), preferred_element_type=jnp.float32
        )
        both = both[: 5 * count] + both[5 * count :]
        for h in range(2):
            at = (g + h) * count
            for t in range(5):
                value = both[t * count : (t + 1) * count, h * LANES : (h + 1) * LANES]
                if t == 4:
                    value = jnp.where(in_block, value, 0.0)
                high, low = split(value)
                high_ref[at : at + count, t * LANES : (t + 1) * LANES] = high
                low_ref[at : at + count, t * LANES : (t + 1) * LANES] = low

    def across(table, ref, start):
        return lax.dot_general(
            table, ref[:, start : start + 2 * LANES], contract, preferred_element_type=jnp.float32
        )

    stores = []
    for w, start in enumerate((0, patch - 2 * LANES)):
        found = across(flat[w], high_ref, start) + across(flat[w], low_ref, start)
        found = found + across(flat[2 + w], high_ref, start)
        part = pl.ds(w * cx // 2, cx // 2)
        dec_ref[part] = found.reshape(cx // 2, cy, depth)
        stores.append(pltpu.make_async_copy(dec_ref.at[part], dec_hbm.at[part], sems.at[w]))
        stores[-1].start()
    edge_ref[...] = across(pick, high_ref, patch) + across(pick, low_ref, patch)

    row = lax.broadcasted_iota(jnp.int32, (cy, depth), 0)
    lane = lax.broadcasted_iota(jnp.int32, (cy, depth), 1)
    total = jnp.zeros((8, LANES), jnp.float32)
    for x in range(cx):
        here = dec_ref[x]
        beside = dec_ref[x - 1] if x > 0 else edge_ref[0:cy]
        beside = beside + (dec_ref[x + 1] if x < cx - 1 else edge_ref[cy : 2 * cy])
        low = edge_ref[2 * cy + x : 2 * cy + x + 1]
        high = edge_ref[2 * cy + cx + x : 2 * cy + cx + x + 1]
        beside = beside + jnp.where(row == 0, low, pltpu.roll(here, 1, 0))
        beside = beside + jnp.where(row == cy - 1, high, pltpu.roll(here, cy - 1, 0))
        beside = beside + jnp.where(lane == 0, 0.0, pltpu.roll(here, 1, 1))
        beside = beside + jnp.where(lane == depth - 1, 0.0, pltpu.roll(here, depth - 1, 1))
        left = right_ref[x] - (6.0 * here - beside)
        res_ref[x] = left
        square = left * left
        for r in range(0, cy, 8):
            for c in range(0, depth, LANES):
                total = total + square[r : r + 8, c : c + LANES]
        if x % 4 == 3:
            part = pl.ds(x - 3, 4)
            stores.append(
                pltpu.make_async_copy(res_ref.at[part], res_hbm.at[part], sems.at[2 + x // 4])
            )
            stores[-1].start()
    total = jnp.sum(total, axis=0, keepdims=True)
    sum_ref[...] = jnp.broadcast_to(total[None], sum_ref.shape)
    for store in stores:
        store.wait()


def finish_kernel(cells, parts_ref, rms_ref):
    total = jnp.sum(parts_ref[...].reshape(-1, LANES), axis=0, keepdims=True)
    total = jnp.sum(total, axis=1, keepdims=True)
    rms_ref[...] = jnp.sqrt(total / cells + 1e-6)


def shards(count_x, count_y, coefficients, exponents, right_side):
    peers = count_x * count_y
    cx, cy, depth = right_side.shape
    patch = cx * cy
    vmem = pl.BlockSpec(memory_space=pltpu.VMEM)
    hbm = pl.BlockSpec(memory_space=pltpu.HBM)
    order = order_of(count_x, count_y)
    tables = jnp.asarray(receive_table(order, cx, cy))
    kept = [(right_side.shape, right_side.dtype), (tables.shape, tables.dtype)]
    kept = [((peers, ROWS // 4, 4, LANES), jnp.bfloat16)] + kept
    held = sum(int(np.prod(shape)) * jnp.dtype(dtype).itemsize for shape, dtype in kept)
    near = held <= 2 << 20
    place = pltpu.VMEM if near else jax.ShapeDtypeStruct
    messages, right_side, tables = pl.pallas_call(
        functools.partial(send_kernel, order, count_x, count_y, cx, cy),
        out_shape=[place(*k) for k in kept],
        in_specs=[hbm] * 5,
        out_specs=[vmem] * 3,
        scratch_shapes=[
            pltpu.VMEM(coefficients.shape, coefficients.dtype),
            pltpu.VMEM(exponents.shape, exponents.dtype),
            pltpu.VMEM((patch, 2 * LANES), jnp.bfloat16),
            pltpu.VMEM((peers * 3, patch), jnp.float32),
            pltpu.VMEM((peers, 16, patch), jnp.bfloat16),
            pltpu.VMEM((peers, 16, LANES), jnp.float32),
            pltpu.SemaphoreType.DMA((5,)),
        ],
        compiler_params=pltpu.CompilerParams(
            vmem_limit_bytes=(64 << 20) - held - (256 << 10) if near else 48 << 20
        ),
        name="send",
    )(
        coefficients,
        exponents,
        jnp.asarray(edge_table(cx, cy)),
        right_side,
        tables,
    )
    got = exchange(messages, order)
    decoded, residual, parts = pl.pallas_call(
        functools.partial(receive_kernel, order, cx, cy),
        out_shape=(
            jax.ShapeDtypeStruct((cx, cy, depth), jnp.float32),
            jax.ShapeDtypeStruct((cx, cy, depth), jnp.float32),
            pltpu.VMEM((peers, 1, LANES), jnp.float32),
        ),
        in_specs=[vmem] * 3,
        out_specs=(hbm, hbm, vmem),
        scratch_shapes=[
            pltpu.VMEM((depth, 5 * LANES), jnp.bfloat16),
            pltpu.VMEM((depth, 5 * LANES), jnp.bfloat16),
            pltpu.VMEM((2 * cx + 2 * cy, depth), jnp.float32),
            pltpu.VMEM((cx, cy, depth), jnp.float32),
            pltpu.VMEM((cx, cy, depth), jnp.float32),
            pltpu.SemaphoreType.DMA((2 + cx // 4,)),
        ],
        compiler_params=pltpu.CompilerParams(vmem_limit_bytes=(12 << 20) * peers // 32),
        name="receive",
    )(got, right_side, tables)
    parts = exchange(parts, order)
    rms = pl.pallas_call(
        functools.partial(finish_kernel, patch * depth * peers),
        out_shape=jax.ShapeDtypeStruct((1, 1), jnp.float32),
        in_specs=[vmem],
        out_specs=vmem,
        compiler_params=pltpu.CompilerParams(vmem_limit_bytes=1 << 20),
        name="finish",
    )(parts)
    return (decoded, residual, rms.reshape(()))


def solution(mesh):
    return jax.shard_map(
        functools.partial(shards, mesh.shape["px"], mesh.shape["py"]),
        mesh=mesh,
        in_specs=(P(AXES, None), P(AXES, None), P("px", "py", None)),
        out_specs=(P("px", "py", None), P("px", "py", None), P()),
        check_vma=False,
    )
```

```python
import functools

import jax
import jax.numpy as jnp
import numpy as np
from jax import lax
from jax.experimental import pallas as pl
from jax.experimental.pallas import tpu as pltpu
from jax.sharding import PartitionSpec as P

AXES = ("px", "py")
LANES = 128
ROWS = 52
TAIL = 48
LAYERS = 12
GROUP = 4
SEQUENCE = (7, 4, 3, 2, 5, 6, 1, 0)
WITHIN = (1, 3, 0, 2)


def order_of(count_x, count_y):
    groups = count_x * count_y // GROUP
    order = SEQUENCE if groups == len(SEQUENCE) else range(groups)
    return [GROUP * g + d for g in order for d in WITHIN]


def exchange(array, order):
    return lax.all_to_all(
        array, AXES, split_axis=0, concat_axis=0, tiled=True, axis_index_groups=[order]
    )


def basis4():
    a = np.arange(4)[:, None]
    i = np.arange(4)[None, :]
    weight = np.where(a == 0, np.sqrt(0.25), np.sqrt(0.5))
    return weight * np.cos(np.pi * (2 * i + 1) * a / 8)


def halves(table):
    table = table.astype(np.float32)
    high = table.astype(jnp.bfloat16)
    low = (table - high.astype(np.float32)).astype(jnp.bfloat16)
    return high, low


def plane(cx, cy):
    across_x = np.kron(np.eye(cx // 4), basis4())
    across_y = np.kron(np.eye(cy // 4), basis4())
    return np.kron(across_x, across_y)


def edge_table(cx, cy):
    full = plane(cx, cy).reshape(cx * cy, cx, cy)
    x_high, x_low = full[:, cx - 1, :], full[:, 0, :]
    y_high, y_low = full[:, :, cy - 1], full[:, :, 0]
    table = np.concatenate([x_high, x_low, y_high, y_low, x_high, x_low], axis=1)
    return np.concatenate(halves(table), axis=1)


def depth_table(order):
    at = np.argsort([d % GROUP for d in order[:GROUP]])
    basis = basis4()
    table = np.zeros((5, GROUP, LAYERS, GROUP, ROWS))
    for s in range(GROUP):
        for point in range(LAYERS):
            block, k = divmod(point, 4)
            for a in range(4):
                layer = 4 * block + a
                for t in range(3):
                    table[t, s, point, at[s], 16 * t + layer] = basis[a, k]
                table[3, s, point, at[s], 16 * block + 12 + a] = basis[a, k]
                table[4, s, point, at[s], TAIL + a] = basis[a, k]
    table = np.concatenate(halves(table.reshape(5 * GROUP * LAYERS, GROUP * ROWS)), axis=1)
    table = np.pad(table, ((0, 0), (0, 4 * LANES - table.shape[1])))
    return np.stack([table[:, : 2 * LANES], table[:, 2 * LANES :]])


def plane_windows(cx, cy):
    flipped = plane(cx, cy).T
    half = cx * cy // 2
    width = 2 * LANES
    first = flipped[:half, :width]
    second = flipped[half:, cx * cy - width :]
    return np.stack(halves(np.stack([first, second])))


def pick_table(cx, cy):
    edges = 2 * cy + 2 * cx
    table = np.zeros((edges, 2 * LANES), np.float32)
    for k in range(2 * cy):
        table[k, k] = 1
        table[k, edges + k] = 1
    for k in range(2 * cx):
        table[2 * cy + k, 2 * cy + k] = 1
        for block in range(3):
            table[2 * cy + k, LANES + 2 * cx * block + k] = 1
    return table.astype(jnp.bfloat16)


def spread_table(cx, cy):
    blocks, patch = cx * cy // 16, cx * cy
    own = lax.broadcasted_iota(jnp.int32, (patch, patch), 0) % blocks
    cell = lax.broadcasted_iota(jnp.int32, (1, patch), 1)
    block = cell // (4 * cy) * (cy // 4) + cell % cy // 4
    return jnp.where(own == block, 1.0, 0.0).astype(jnp.bfloat16)


def send_kernel(
    order, count_x, count_y, cx, cy, coef_hbm, exp_hbm, edge_hbm, right_hbm, table_hbm,
    out_ref, right_ref, table_ref, coef_ref, exp_ref, edge_ref, factor, scaled, edge, sems,
):
    pairs = [(exp_hbm, exp_ref), (coef_hbm, coef_ref), (edge_hbm, edge_ref)]
    pairs += [(right_hbm, right_ref), (table_hbm, table_ref)]
    loads = [pltpu.make_async_copy(a, b, sems.at[n]) for n, (a, b) in enumerate(pairs)]
    for load in loads:
        load.start()
    peers = count_x * count_y
    place = np.argsort(order)
    patch = cx * cy
    blocks = patch // 16
    per = patch // blocks
    edges = 2 * cy + 2 * cx
    spread = spread_table(cx, cy)
    loads[0].wait()
    power = lax.shift_left(jnp.int32(1), exp_ref[...] + 15).astype(jnp.float32) * (2.0**-15)
    lane = lax.broadcasted_iota(jnp.int32, (per, patch), 1)
    row = lax.broadcasted_iota(jnp.int32, (per, patch), 0)
    own = (lane >= row * blocks) & (lane < (row + 1) * blocks)
    for h in range(peers // per):
        part = power[:, h * patch : (h + 1) * patch]
        stacked = [
            jnp.where(own, jnp.broadcast_to(part[b : b + 1], (per, patch)), 0.0) for b in range(3)
        ]
        left = jnp.concatenate(stacked, axis=0).astype(jnp.bfloat16)
        factor[h * 3 * per : (h + 1) * 3 * per, :] = jnp.dot(
            left, spread, preferred_element_type=jnp.float32
        )
    layer = lax.broadcasted_iota(jnp.int32, (LAYERS, patch), 0)
    wide = lax.broadcasted_iota(jnp.int32, (4, LANES), 1)
    lane = lax.broadcasted_iota(jnp.int32, (16, LANES), 1)
    from_left = (lane < cy) | ((lane >= edges) & (lane < edges + cy))
    from_right = ((lane >= cy) & (lane < 2 * cy)) | (lane >= edges + cy)
    from_below = (lane >= 2 * cy) & (lane < 2 * cy + cx)
    nothing = jnp.zeros((16, LANES), jnp.float32)

    for p in range(peers):
        base = p // per * 3 * per + p % per
        rows = [
            jnp.broadcast_to(factor[base + b * per : base + b * per + 1, :], (LAYERS, patch))
            for b in range(3)
        ]
        scale = jnp.where(layer < 4, rows[0], jnp.where(layer < 8, rows[1], rows[2]))
        scaled[p, 0:LAYERS, :] = scale.astype(jnp.bfloat16)

    def scale_row(i):
        for p in range(i * count_y, (i + 1) * count_y):
            part = coef_ref[:, p * patch : (p + 1) * patch] * scaled[p, 0:LAYERS, :]
            scaled[p, 0:LAYERS, :] = part
            for t in range(3):
                tile = part[:, t * LANES : (t + 1) * LANES]
                for k in range(3):
                    out_ref[place[p], 4 * t + k] = tile[4 * k : 4 * k + 4]
        row = pl.ds(i * count_y, count_y)
        found = jnp.dot(
            scaled[row].reshape(count_y * 16, patch),
            edge_ref[...],
            preferred_element_type=jnp.float32,
        )
        edge[row] = (found[:, :LANES] + found[:, LANES:]).reshape(count_y, 16, LANES)

    def join_row(i):
        for p in range(i * count_y, (i + 1) * count_y):
            j = p % count_y
            left = edge[p - count_y] if i > 0 else nothing
            right = edge[p + count_y] if i < count_x - 1 else nothing
            below = edge[p - 1] if j > 0 else nothing
            above = edge[p + 1] if j < count_y - 1 else nothing
            value = jnp.where(
                from_left, left, jnp.where(from_right, right, jnp.where(from_below, below, above))
            )
            high = value.astype(jnp.bfloat16).astype(jnp.float32)
            low = value - high
            tile = jnp.where(lane < edges, high, low).astype(jnp.bfloat16)
            for t in range(3):
                out_ref[place[p], 4 * t + 3] = tile[4 * t : 4 * t + 4]
            first = pltpu.roll(low[0:8], LANES - 2 * cy, 1)[0:4]
            second = pltpu.roll(low[0:8], LANES - 2 * cy + 2 * cx, 1)[4:8]
            third = pltpu.roll(low[8:16], (4 * cx - 2 * cy) % LANES, 1)[0:4]
            tail = jnp.where(wide < 2 * cx, first, jnp.where(wide < 4 * cx, second, third))
            tail = jnp.where(wide < 6 * cx, tail, 0.0)
            out_ref[place[p], TAIL // 4] = tail.astype(jnp.bfloat16)

    loads[1].wait()
    loads[2].wait()
    for i in range(count_x):
        scale_row(i)
        if i > 0:
            join_row(i - 1)
    join_row(count_x - 1)
    loads[3].wait()
    loads[4].wait()


def receive_table(order, cx, cy):
    parts = [depth_table(order), plane_windows(cx, cy), pick_table(cx, cy)]
    return np.concatenate([part.reshape(-1, 2 * LANES) for part in parts], axis=0)


def split(value):
    high = value.astype(jnp.bfloat16)
    return high, (value - high.astype(jnp.float32)).astype(jnp.bfloat16)


def receive_kernel(
    order, cx, cy, got_ref, right_ref, table_ref, dec_hbm, res_hbm, sum_ref,
    high_ref, low_ref, edge_ref, dec_ref, res_ref, sems,
):
    peers = got_ref.shape[0]
    groups = np.argsort([d // GROUP for d in order[::GROUP]])
    depth = peers * LAYERS
    patch = cx * cy
    count = GROUP * LAYERS
    half = patch // 2
    starts = [0, 5 * count, 10 * count] + [10 * count + half * n for n in range(1, 5)]
    starts = starts + [table_ref.shape[0]]
    table = [table_ref[a:b] for a, b in zip(starts[:-1], starts[1:])]
    deep = jnp.concatenate(table[:2], axis=1)[:, : 2 * GROUP * ROWS]
    row = lax.broadcasted_iota(jnp.int32, (count, LANES), 0)
    lane = lax.broadcasted_iota(jnp.int32, (count, LANES), 1)
    third = 2 * cx
    block = row // 4 % 3
    in_block = (lane >= block * third) & (lane < (block + 1) * third)
    for g in range(0, peers // GROUP, 2):
        both = jnp.concatenate(
            [
                got_ref[GROUP * h : GROUP * (h + 1)].reshape(GROUP * ROWS, LANES)
                for h in (groups[g], groups[g + 1])
            ],
            axis=1,
        )
        both = jnp.dot(
            deep, jnp.concatenate([both, both], axis=0), preferred_element_type=jnp.float32
        )
        for h in range(2):
            at = (g + h) * count
            for t in range(5):
                value = both[t * count : (t + 1) * count, h * LANES : (h + 1) * LANES]
                if t == 4:
                    value = jnp.where(in_block, value, 0.0)
                high, low = split(value)
                high_ref[at : at + count, t * LANES : (t + 1) * LANES] = high
                low_ref[at : at + count, t * LANES : (t + 1) * LANES] = low

    def across(tables, refs, start):
        return lax.dot_general(
            jnp.concatenate(tables, axis=1),
            jnp.concatenate([ref[:, start : start + 2 * LANES] for ref in refs], axis=1),
            (((1,), (1,)), ((), ())),
            preferred_element_type=jnp.float32,
        )

    row = lax.broadcasted_iota(jnp.int32, (cy, depth), 0)
    lane = lax.broadcasted_iota(jnp.int32, (cy, depth), 1)
    stores = []

    def store(source, target):
        stores.append(pltpu.make_async_copy(source, target, sems.at[len(stores)]))
        stores[-1].start()

    def decode(w, start):
        found = across(
            [table[2 + w], table[2 + w], table[4 + w]], [high_ref, low_ref, high_ref], start
        )
        part = pl.ds(w * cx // 2, cx // 2)
        dec_ref[part] = found.reshape(cx // 2, cy, depth)
        store(dec_ref.at[part], dec_hbm.at[part])

    def finish(x, total):
        here = dec_ref[x]
        beside = dec_ref[x - 1] if x > 0 else edge_ref[0:cy]
        beside = beside + (dec_ref[x + 1] if x < cx - 1 else edge_ref[cy : 2 * cy])
        low = edge_ref[2 * cy + x : 2 * cy + x + 1]
        high = edge_ref[2 * cy + cx + x : 2 * cy + cx + x + 1]
        beside = beside + jnp.where(row == 0, low, pltpu.roll(here, 1, 0))
        beside = beside + jnp.where(row == cy - 1, high, pltpu.roll(here, cy - 1, 0))
        beside = beside + jnp.where(lane == 0, 0.0, pltpu.roll(here, 1, 1))
        beside = beside + jnp.where(lane == depth - 1, 0.0, pltpu.roll(here, depth - 1, 1))
        left = right_ref[x] - (6.0 * here - beside)
        res_ref[x] = left
        square = left * left
        for r in range(0, cy, 8):
            for c in range(0, depth, LANES):
                total = total + square[r : r + 8, c : c + LANES]
        if x % 4 == 3:
            part = pl.ds(x - 3, 4)
            store(res_ref.at[part], res_hbm.at[part])
        return total

    total = jnp.zeros((8, LANES), jnp.float32)
    decode(0, 0)
    edge_ref[...] = across([table[6], table[6]], [high_ref, low_ref], patch)
    for x in range(cx // 2 - 1):
        total = finish(x, total)
    decode(1, patch - 2 * LANES)
    for x in range(cx // 2 - 1, cx):
        total = finish(x, total)
    total = jnp.sum(total, axis=0, keepdims=True)
    sum_ref[...] = jnp.broadcast_to(total[None], sum_ref.shape)
    for copy in stores:
        copy.wait()


def finish_kernel(cells, parts_ref, rms_ref):
    total = jnp.sum(parts_ref[...].reshape(-1, LANES), axis=0, keepdims=True)
    total = jnp.sum(total, axis=1, keepdims=True)
    rms_ref[...] = jnp.sqrt(total / cells + 1e-6)


def shards(count_x, count_y, coefficients, exponents, right_side):
    peers = count_x * count_y
    cx, cy, depth = right_side.shape
    patch = cx * cy
    vmem = pl.BlockSpec(memory_space=pltpu.VMEM)
    hbm = pl.BlockSpec(memory_space=pltpu.HBM)
    order = order_of(count_x, count_y)
    tables = jnp.asarray(receive_table(order, cx, cy))
    kept = [(right_side.shape, right_side.dtype), (tables.shape, tables.dtype)]
    kept = [((peers, ROWS // 4, 4, LANES), jnp.bfloat16)] + kept
    held = sum(int(np.prod(shape)) * jnp.dtype(dtype).itemsize for shape, dtype in kept)
    near = held <= 2 << 20
    place = pltpu.VMEM if near else jax.ShapeDtypeStruct
    messages, right_side, tables = pl.pallas_call(
        functools.partial(send_kernel, order, count_x, count_y, cx, cy),
        out_shape=[place(*k) for k in kept],
        in_specs=[hbm] * 5,
        out_specs=[vmem] * 3,
        scratch_shapes=[
            pltpu.VMEM(coefficients.shape, coefficients.dtype),
            pltpu.VMEM(exponents.shape, exponents.dtype),
            pltpu.VMEM((patch, 2 * LANES), jnp.bfloat16),
            pltpu.VMEM((peers * 3, patch), jnp.float32),
            pltpu.VMEM((peers, 16, patch), jnp.bfloat16),
            pltpu.VMEM((peers, 16, LANES), jnp.float32),
            pltpu.SemaphoreType.DMA((5,)),
        ],
        compiler_params=pltpu.CompilerParams(
            vmem_limit_bytes=(64 << 20) - held - (256 << 10) if near else 48 << 20
        ),
        name="send",
    )(
        coefficients,
        exponents,
        jnp.asarray(edge_table(cx, cy)),
        right_side,
        tables,
    )
    got = exchange(messages, order)
    decoded, residual, parts = pl.pallas_call(
        functools.partial(receive_kernel, order, cx, cy),
        out_shape=(
            jax.ShapeDtypeStruct((cx, cy, depth), jnp.float32),
            jax.ShapeDtypeStruct((cx, cy, depth), jnp.float32),
            pltpu.VMEM((peers, 1, LANES), jnp.float32),
        ),
        in_specs=[vmem] * 3,
        out_specs=(hbm, hbm, vmem),
        scratch_shapes=[
            pltpu.VMEM((depth, 5 * LANES), jnp.bfloat16),
            pltpu.VMEM((depth, 5 * LANES), jnp.bfloat16),
            pltpu.VMEM((2 * cx + 2 * cy, depth), jnp.float32),
            pltpu.VMEM((cx, cy, depth), jnp.float32),
            pltpu.VMEM((cx, cy, depth), jnp.float32),
            pltpu.SemaphoreType.DMA((2 + cx // 4,)),
        ],
        compiler_params=pltpu.CompilerParams(vmem_limit_bytes=(12 << 20) * peers // 32),
        name="receive",
    )(got, right_side, tables)
    parts = exchange(parts, order)
    rms = pl.pallas_call(
        functools.partial(finish_kernel, patch * depth * peers),
        out_shape=jax.ShapeDtypeStruct((1, 1), jnp.float32),
        in_specs=[vmem],
        out_specs=vmem,
        compiler_params=pltpu.CompilerParams(vmem_limit_bytes=1 << 20),
        name="finish",
    )(parts)
    return (decoded, residual, rms.reshape(()))


def solution(mesh):
    return jax.shard_map(
        functools.partial(shards, mesh.shape["px"], mesh.shape["py"]),
        mesh=mesh,
        in_specs=(P(AXES, None), P(AXES, None), P("px", "py", None)),
        out_specs=(P("px", "py", None), P("px", "py", None), P()),
        check_vma=False,
    )
```

```python
import functools

import jax
import jax.numpy as jnp
import numpy as np
from jax import lax
from jax.experimental import pallas as pl
from jax.experimental.pallas import tpu as pltpu
from jax.sharding import PartitionSpec as P

AXES = ("px", "py")
LANES = 128
ROWS = 52
TAIL = 48
LAYERS = 12
GROUP = 4
SEQUENCE = (7, 4, 3, 2, 5, 6, 1, 0)
WITHIN = (1, 3, 0, 2)


def order_of(count_x, count_y):
    groups = count_x * count_y // GROUP
    order = SEQUENCE if groups == len(SEQUENCE) else range(groups)
    return [GROUP * g + d for g in order for d in WITHIN]


def exchange(array, order):
    return lax.all_to_all(
        array, AXES, split_axis=0, concat_axis=0, tiled=True, axis_index_groups=[order]
    )


def basis4():
    a = np.arange(4)[:, None]
    i = np.arange(4)[None, :]
    weight = np.where(a == 0, np.sqrt(0.25), np.sqrt(0.5))
    return weight * np.cos(np.pi * (2 * i + 1) * a / 8)


def halves(table):
    table = table.astype(np.float32)
    high = table.astype(jnp.bfloat16)
    low = (table - high.astype(np.float32)).astype(jnp.bfloat16)
    return high, low


def plane(cx, cy):
    across_x = np.kron(np.eye(cx // 4), basis4())
    across_y = np.kron(np.eye(cy // 4), basis4())
    return np.kron(across_x, across_y)


def edge_table(cx, cy):
    full = plane(cx, cy).reshape(cx * cy, cx, cy)
    x_high, x_low = full[:, cx - 1, :], full[:, 0, :]
    y_high, y_low = full[:, :, cy - 1], full[:, :, 0]
    table = np.concatenate([x_high, x_low, y_high, y_low, x_high, x_low], axis=1)
    return np.concatenate(halves(table), axis=1)


def depth_table(order):
    at = np.argsort([d % GROUP for d in order[:GROUP]])
    basis = basis4()
    table = np.zeros((5, GROUP, LAYERS, GROUP, ROWS))
    for s in range(GROUP):
        for point in range(LAYERS):
            block, k = divmod(point, 4)
            for a in range(4):
                layer = 4 * block + a
                for t in range(3):
                    table[t, s, point, at[s], 16 * t + layer] = basis[a, k]
                table[3, s, point, at[s], 16 * block + 12 + a] = basis[a, k]
                table[4, s, point, at[s], TAIL + a] = basis[a, k]
    table = np.concatenate(halves(table.reshape(5 * GROUP * LAYERS, GROUP * ROWS)), axis=1)
    table = np.pad(table, ((0, 0), (0, 4 * LANES - table.shape[1])))
    return np.stack([table[:, : 2 * LANES], table[:, 2 * LANES :]])


def plane_windows(cx, cy):
    flipped = plane(cx, cy).T
    half = cx * cy // 2
    width = 2 * LANES
    first = flipped[:half, :width]
    second = flipped[half:, cx * cy - width :]
    return np.stack(halves(np.stack([first, second])))


def pick_table(cx, cy):
    edges = 2 * cy + 2 * cx
    table = np.zeros((edges, 2 * LANES), np.float32)
    for k in range(2 * cy):
        table[k, k] = 1
        table[k, edges + k] = 1
    for k in range(2 * cx):
        table[2 * cy + k, 2 * cy + k] = 1
        for block in range(3):
            table[2 * cy + k, LANES + 2 * cx * block + k] = 1
    return table.astype(jnp.bfloat16)


def spread_table(cx, cy):
    blocks, patch = cx * cy // 16, cx * cy
    own = lax.broadcasted_iota(jnp.int32, (patch, patch), 0) % blocks
    cell = lax.broadcasted_iota(jnp.int32, (1, patch), 1)
    block = cell // (4 * cy) * (cy // 4) + cell % cy // 4
    return jnp.where(own == block, 1.0, 0.0).astype(jnp.bfloat16)


def send_kernel(
    order, count_x, count_y, cx, cy, coef_hbm, exp_hbm, edge_hbm, right_hbm, table_hbm,
    out_ref, right_ref, table_ref, coef_ref, exp_ref, edge_ref, factor, scaled, edge, sems,
):
    pairs = [(exp_hbm, exp_ref), (coef_hbm, coef_ref), (edge_hbm, edge_ref)]
    pairs += [(right_hbm, right_ref), (table_hbm, table_ref)]
    loads = [pltpu.make_async_copy(a, b, sems.at[n]) for n, (a, b) in enumerate(pairs)]
    for load in loads:
        load.start()
    peers = count_x * count_y
    place = np.argsort(order)
    patch = cx * cy
    blocks = patch // 16
    per = patch // blocks
    edges = 2 * cy + 2 * cx
    spread = spread_table(cx, cy)
    loads[0].wait()
    power = lax.shift_left(jnp.int32(1), exp_ref[...] + 15).astype(jnp.float32) * (2.0**-15)
    lane = lax.broadcasted_iota(jnp.int32, (per, patch), 1)
    row = lax.broadcasted_iota(jnp.int32, (per, patch), 0)
    own = (lane >= row * blocks) & (lane < (row + 1) * blocks)
    for h in range(peers // per):
        part = power[:, h * patch : (h + 1) * patch]
        stacked = [
            jnp.where(own, jnp.broadcast_to(part[b : b + 1], (per, patch)), 0.0) for b in range(3)
        ]
        left = jnp.concatenate(stacked, axis=0).astype(jnp.bfloat16)
        factor[h * 3 * per : (h + 1) * 3 * per, :] = jnp.dot(
            left, spread, preferred_element_type=jnp.float32
        )
    layer = lax.broadcasted_iota(jnp.int32, (LAYERS, patch), 0)
    wide = lax.broadcasted_iota(jnp.int32, (4, LANES), 1)
    lane = lax.broadcasted_iota(jnp.int32, (16, LANES), 1)
    from_left = (lane < cy) | ((lane >= edges) & (lane < edges + cy))
    from_right = ((lane >= cy) & (lane < 2 * cy)) | (lane >= edges + cy)
    from_below = (lane >= 2 * cy) & (lane < 2 * cy + cx)
    nothing = jnp.zeros((16, LANES), jnp.float32)

    for p in range(peers):
        base = p // per * 3 * per + p % per
        rows = [
            jnp.broadcast_to(factor[base + b * per : base + b * per + 1, :], (LAYERS, patch))
            for b in range(3)
        ]
        scale = jnp.where(layer < 4, rows[0], jnp.where(layer < 8, rows[1], rows[2]))
        scaled[p, 0:LAYERS, :] = scale.astype(jnp.bfloat16)

    def scale_row(i):
        for p in range(i * count_y, (i + 1) * count_y):
            part = coef_ref[:, p * patch : (p + 1) * patch] * scaled[p, 0:LAYERS, :]
            scaled[p, 0:LAYERS, :] = part
            for t in range(3):
                tile = part[:, t * LANES : (t + 1) * LANES]
                for k in range(3):
                    out_ref[place[p], 4 * t + k] = tile[4 * k : 4 * k + 4]
        row = pl.ds(i * count_y, count_y)
        found = jnp.dot(
            scaled[row].reshape(count_y * 16, patch),
            edge_ref[...],
            preferred_element_type=jnp.float32,
        )
        edge[row] = (found[:, :LANES] + found[:, LANES:]).reshape(count_y, 16, LANES)

    def join_row(i):
        for p in range(i * count_y, (i + 1) * count_y):
            j = p % count_y
            left = edge[p - count_y] if i > 0 else nothing
            right = edge[p + count_y] if i < count_x - 1 else nothing
            below = edge[p - 1] if j > 0 else nothing
            above = edge[p + 1] if j < count_y - 1 else nothing
            value = jnp.where(
                from_left, left, jnp.where(from_right, right, jnp.where(from_below, below, above))
            )
            high = value.astype(jnp.bfloat16).astype(jnp.float32)
            low = value - high
            tile = jnp.where(lane < edges, high, low).astype(jnp.bfloat16)
            for t in range(3):
                out_ref[place[p], 4 * t + 3] = tile[4 * t : 4 * t + 4]
            first = pltpu.roll(low[0:8], LANES - 2 * cy, 1)[0:4]
            second = pltpu.roll(low[0:8], LANES - 2 * cy + 2 * cx, 1)[4:8]
            third = pltpu.roll(low[8:16], (4 * cx - 2 * cy) % LANES, 1)[0:4]
            tail = jnp.where(wide < 2 * cx, first, jnp.where(wide < 4 * cx, second, third))
            tail = jnp.where(wide < 6 * cx, tail, 0.0)
            out_ref[place[p], TAIL // 4] = tail.astype(jnp.bfloat16)

    loads[1].wait()
    loads[2].wait()
    for i in range(count_x):
        scale_row(i)
        if i > 0:
            join_row(i - 1)
    join_row(count_x - 1)
    loads[3].wait()
    loads[4].wait()


def receive_table(order, cx, cy):
    parts = [depth_table(order), plane_windows(cx, cy), pick_table(cx, cy)]
    return np.concatenate([part.reshape(-1, 2 * LANES) for part in parts], axis=0)


def split(value):
    high = value.astype(jnp.bfloat16)
    return high, (value - high.astype(jnp.float32)).astype(jnp.bfloat16)


def receive_kernel(
    late, order, cx, cy, got_ref, right_ref, table_ref, dec_hbm, res_hbm, late_ref, sum_ref,
    high_ref, low_ref, edge_ref, dec_ref, res_ref, sems,
):
    peers = got_ref.shape[0]
    groups = np.argsort([d // GROUP for d in order[::GROUP]])
    depth = peers * LAYERS
    patch = cx * cy
    count = GROUP * LAYERS
    half = patch // 2
    starts = [0, 5 * count, 10 * count] + [10 * count + half * n for n in range(1, 5)]
    starts = starts + [table_ref.shape[0]]
    table = [table_ref[a:b] for a, b in zip(starts[:-1], starts[1:])]
    deep = jnp.concatenate(table[:2], axis=1)[:, : 2 * GROUP * ROWS]
    row = lax.broadcasted_iota(jnp.int32, (count, LANES), 0)
    lane = lax.broadcasted_iota(jnp.int32, (count, LANES), 1)
    third = 2 * cx
    block = row // 4 % 3
    in_block = (lane >= block * third) & (lane < (block + 1) * third)
    for g in range(0, peers // GROUP, 2):
        both = jnp.concatenate(
            [
                got_ref[GROUP * h : GROUP * (h + 1)].reshape(GROUP * ROWS, LANES)
                for h in (groups[g], groups[g + 1])
            ],
            axis=1,
        )
        both = jnp.dot(
            deep, jnp.concatenate([both, both], axis=0), preferred_element_type=jnp.float32
        )
        for h in range(2):
            at = (g + h) * count
            for t in range(5):
                value = both[t * count : (t + 1) * count, h * LANES : (h + 1) * LANES]
                if t == 4:
                    value = jnp.where(in_block, value, 0.0)
                high, low = split(value)
                high_ref[at : at + count, t * LANES : (t + 1) * LANES] = high
                low_ref[at : at + count, t * LANES : (t + 1) * LANES] = low

    def across(tables, refs, start):
        return lax.dot_general(
            jnp.concatenate(tables, axis=1),
            jnp.concatenate([ref[:, start : start + 2 * LANES] for ref in refs], axis=1),
            (((1,), (1,)), ((), ())),
            preferred_element_type=jnp.float32,
        )

    row = lax.broadcasted_iota(jnp.int32, (cy, depth), 0)
    lane = lax.broadcasted_iota(jnp.int32, (cy, depth), 1)
    stores = []

    def store(source, target):
        stores.append(pltpu.make_async_copy(source, target, sems.at[len(stores)]))
        stores[-1].start()

    def decode(w, start):
        found = across(
            [table[2 + w], table[2 + w], table[4 + w]], [high_ref, low_ref, high_ref], start
        )
        part = pl.ds(w * cx // 2, cx // 2)
        dec_ref[part] = found.reshape(cx // 2, cy, depth)
        store(dec_ref.at[part], dec_hbm.at[part])

    def finish(x, total):
        here = dec_ref[x]
        beside = dec_ref[x - 1] if x > 0 else edge_ref[0:cy]
        beside = beside + (dec_ref[x + 1] if x < cx - 1 else edge_ref[cy : 2 * cy])
        low = edge_ref[2 * cy + x : 2 * cy + x + 1]
        high = edge_ref[2 * cy + cx + x : 2 * cy + cx + x + 1]
        beside = beside + jnp.where(row == 0, low, pltpu.roll(here, 1, 0))
        beside = beside + jnp.where(row == cy - 1, high, pltpu.roll(here, cy - 1, 0))
        beside = beside + jnp.where(lane == 0, 0.0, pltpu.roll(here, 1, 1))
        beside = beside + jnp.where(lane == depth - 1, 0.0, pltpu.roll(here, depth - 1, 1))
        left = right_ref[x] - (6.0 * here - beside)
        if x < late:
            res_ref[x] = left
        else:
            late_ref[x - late] = left
        square = left * left
        for r in range(0, cy, 8):
            for c in range(0, depth, LANES):
                total = total + square[r : r + 8, c : c + LANES]
        if x % 4 == 3 and x < late:
            part = pl.ds(x - 3, 4)
            store(res_ref.at[part], res_hbm.at[part])
        return total

    total = jnp.zeros((8, LANES), jnp.float32)
    decode(0, 0)
    edge_ref[...] = across([table[6], table[6]], [high_ref, low_ref], patch)
    for x in range(cx // 2 - 1):
        total = finish(x, total)
    decode(1, patch - 2 * LANES)
    for x in range(cx // 2 - 1, cx):
        total = finish(x, total)
    total = jnp.sum(total, axis=0, keepdims=True)
    sum_ref[...] = jnp.broadcast_to(total[None], sum_ref.shape)
    for copy in stores:
        copy.wait()


def finish_kernel(cells, late, parts_ref, late_ref, res_in, rms_hbm, res_hbm, rms_ref, sems):
    part = pl.ds(late, late_ref.shape[0])
    stores = [pltpu.make_async_copy(late_ref, res_hbm.at[part], sems.at[0])]
    stores += [pltpu.make_async_copy(rms_ref, rms_hbm, sems.at[1])]
    stores[0].start()
    total = jnp.sum(parts_ref[...].reshape(-1, LANES), axis=0, keepdims=True)
    total = jnp.sum(total, axis=1, keepdims=True)
    rms_ref[...] = jnp.sqrt(total / cells + 1e-6)
    stores[1].start()
    for copy in stores:
        copy.wait()


def shards(count_x, count_y, coefficients, exponents, right_side):
    peers = count_x * count_y
    cx, cy, depth = right_side.shape
    patch = cx * cy
    vmem = pl.BlockSpec(memory_space=pltpu.VMEM)
    hbm = pl.BlockSpec(memory_space=pltpu.HBM)
    order = order_of(count_x, count_y)
    tables = jnp.asarray(receive_table(order, cx, cy))
    kept = [(right_side.shape, right_side.dtype), (tables.shape, tables.dtype)]
    kept = [((peers, ROWS // 4, 4, LANES), jnp.bfloat16)] + kept
    held = sum(int(np.prod(shape)) * jnp.dtype(dtype).itemsize for shape, dtype in kept)
    near = held <= 2 << 20
    place = pltpu.VMEM if near else jax.ShapeDtypeStruct
    messages, right_side, tables = pl.pallas_call(
        functools.partial(send_kernel, order, count_x, count_y, cx, cy),
        out_shape=[place(*k) for k in kept],
        in_specs=[hbm] * 5,
        out_specs=[vmem] * 3,
        scratch_shapes=[
            pltpu.VMEM(coefficients.shape, coefficients.dtype),
            pltpu.VMEM(exponents.shape, exponents.dtype),
            pltpu.VMEM((patch, 2 * LANES), jnp.bfloat16),
            pltpu.VMEM((peers * 3, patch), jnp.float32),
            pltpu.VMEM((peers, 16, patch), jnp.bfloat16),
            pltpu.VMEM((peers, 16, LANES), jnp.float32),
            pltpu.SemaphoreType.DMA((5,)),
        ],
        compiler_params=pltpu.CompilerParams(
            vmem_limit_bytes=(64 << 20) - held - (256 << 10) if near else 48 << 20
        ),
        name="send",
    )(
        coefficients,
        exponents,
        jnp.asarray(edge_table(cx, cy)),
        right_side,
        tables,
    )
    got = exchange(messages, order)
    field = jax.ShapeDtypeStruct((cx, cy, depth), jnp.float32)
    late = cx - cx // 4
    decoded, residual, rest, parts = pl.pallas_call(
        functools.partial(receive_kernel, late, order, cx, cy),
        out_shape=(
            field,
            field,
            pltpu.VMEM((cx - late, cy, depth), jnp.float32),
            pltpu.VMEM((peers, 1, LANES), jnp.float32),
        ),
        in_specs=[vmem] * 3,
        out_specs=(hbm, hbm, vmem, vmem),
        scratch_shapes=[
            pltpu.VMEM((depth, 5 * LANES), jnp.bfloat16),
            pltpu.VMEM((depth, 5 * LANES), jnp.bfloat16),
            pltpu.VMEM((2 * cx + 2 * cy, depth), jnp.float32),
            pltpu.VMEM((cx, cy, depth), jnp.float32),
            pltpu.VMEM((late, cy, depth), jnp.float32),
            pltpu.SemaphoreType.DMA((2 + late // 4,)),
        ],
        compiler_params=pltpu.CompilerParams(vmem_limit_bytes=(12 << 20) * peers // 32),
        name="receive",
    )(got, right_side, tables)
    parts = exchange(parts, order)
    rms, residual = pl.pallas_call(
        functools.partial(finish_kernel, patch * depth * peers, late),
        out_shape=(jax.ShapeDtypeStruct((1, 1), jnp.float32), field),
        in_specs=[vmem, vmem, hbm],
        out_specs=(hbm, hbm),
        input_output_aliases={2: 1},
        scratch_shapes=[pltpu.VMEM((1, 1), jnp.float32), pltpu.SemaphoreType.DMA((2,))],
        compiler_params=pltpu.CompilerParams(vmem_limit_bytes=1 << 20),
        name="finish",
    )(parts, rest, residual)
    return (decoded, residual, rms.reshape(()))


def solution(mesh):
    return jax.shard_map(
        functools.partial(shards, mesh.shape["px"], mesh.shape["py"]),
        mesh=mesh,
        in_specs=(P(AXES, None), P(AXES, None), P("px", "py", None)),
        out_specs=(P("px", "py", None), P("px", "py", None), P()),
        check_vma=False,
    )
```

```python
import functools

import jax
import jax.numpy as jnp
import numpy as np
from jax import lax
from jax.experimental import pallas as pl
from jax.experimental.pallas import tpu as pltpu
from jax.sharding import PartitionSpec as P

AXES = ("px", "py")
LANES = 128
ROWS = 52
TAIL = 48
LAYERS = 12
GROUP = 4
SEQUENCE = (7, 4, 3, 2, 5, 6, 1, 0)
WITHIN = (1, 3, 0, 2)


def order_of(count_x, count_y):
    groups = count_x * count_y // GROUP
    order = SEQUENCE if groups == len(SEQUENCE) else range(groups)
    return [GROUP * g + d for g in order for d in WITHIN]


def exchange(array, order):
    return lax.all_to_all(
        array, AXES, split_axis=0, concat_axis=0, tiled=True, axis_index_groups=[order]
    )


def basis4():
    a = np.arange(4)[:, None]
    i = np.arange(4)[None, :]
    weight = np.where(a == 0, np.sqrt(0.25), np.sqrt(0.5))
    return weight * np.cos(np.pi * (2 * i + 1) * a / 8)


def halves(table):
    table = table.astype(np.float32)
    high = table.astype(jnp.bfloat16)
    low = (table - high.astype(np.float32)).astype(jnp.bfloat16)
    return high, low


def plane(cx, cy):
    across_x = np.kron(np.eye(cx // 4), basis4())
    across_y = np.kron(np.eye(cy // 4), basis4())
    return np.kron(across_x, across_y)


def edge_table(cx, cy):
    full = plane(cx, cy).reshape(cx * cy, cx, cy)
    x_high, x_low = full[:, cx - 1, :], full[:, 0, :]
    y_high, y_low = full[:, :, cy - 1], full[:, :, 0]
    table = np.concatenate([x_high, x_low, y_high, y_low, x_high, x_low], axis=1)
    return np.concatenate(halves(table), axis=1)


def depth_table(order):
    at = np.argsort([d % GROUP for d in order[:GROUP]])
    basis = basis4()
    table = np.zeros((5, GROUP, LAYERS, GROUP, ROWS))
    for s in range(GROUP):
        for point in range(LAYERS):
            block, k = divmod(point, 4)
            for a in range(4):
                layer = 4 * block + a
                for t in range(3):
                    table[t, s, point, at[s], 16 * t + layer] = basis[a, k]
                table[3, s, point, at[s], 16 * block + 12 + a] = basis[a, k]
                table[4, s, point, at[s], TAIL + a] = basis[a, k]
    table = np.concatenate(halves(table.reshape(5 * GROUP * LAYERS, GROUP * ROWS)), axis=1)
    table = np.pad(table, ((0, 0), (0, 4 * LANES - table.shape[1])))
    return np.stack([table[:, : 2 * LANES], table[:, 2 * LANES :]])


def plane_windows(cx, cy):
    flipped = plane(cx, cy).T
    half = cx * cy // 2
    width = 2 * LANES
    first = flipped[:half, :width]
    second = flipped[half:, cx * cy - width :]
    return np.stack(halves(np.stack([first, second])))


def pick_table(cx, cy):
    edges = 2 * cy + 2 * cx
    table = np.zeros((edges, 2 * LANES), np.float32)
    for k in range(2 * cy):
        table[k, k] = 1
        table[k, edges + k] = 1
    for k in range(2 * cx):
        table[2 * cy + k, 2 * cy + k] = 1
        for block in range(3):
            table[2 * cy + k, LANES + 2 * cx * block + k] = 1
    return table.astype(jnp.bfloat16)


def spread_table(cx, cy):
    blocks, patch = cx * cy // 16, cx * cy
    own = lax.broadcasted_iota(jnp.int32, (patch, patch), 0) % blocks
    cell = lax.broadcasted_iota(jnp.int32, (1, patch), 1)
    block = cell // (4 * cy) * (cy // 4) + cell % cy // 4
    return jnp.where(own == block, 1.0, 0.0).astype(jnp.bfloat16)


def send_kernel(
    order, count_x, count_y, cx, cy, coef_hbm, exp_hbm, edge_hbm, right_hbm, table_hbm,
    out_ref, right_ref, table_ref, coef_ref, exp_ref, edge_ref, factor, scaled, edge, sems,
):
    pairs = [(exp_hbm, exp_ref), (coef_hbm, coef_ref), (edge_hbm, edge_ref)]
    pairs += [(right_hbm, right_ref), (table_hbm, table_ref)]
    loads = [pltpu.make_async_copy(a, b, sems.at[n]) for n, (a, b) in enumerate(pairs)]
    for load in loads:
        load.start()
    peers = count_x * count_y
    place = np.argsort(order)
    patch = cx * cy
    blocks = patch // 16
    per = patch // blocks
    edges = 2 * cy + 2 * cx
    spread = spread_table(cx, cy)
    loads[0].wait()
    power = lax.shift_left(jnp.int32(1), exp_ref[...] + 15).astype(jnp.float32) * (2.0**-15)
    lane = lax.broadcasted_iota(jnp.int32, (per, patch), 1)
    row = lax.broadcasted_iota(jnp.int32, (per, patch), 0)
    own = (lane >= row * blocks) & (lane < (row + 1) * blocks)
    for h in range(peers // per):
        part = power[:, h * patch : (h + 1) * patch]
        stacked = [
            jnp.where(own, jnp.broadcast_to(part[b : b + 1], (per, patch)), 0.0) for b in range(3)
        ]
        left = jnp.concatenate(stacked, axis=0).astype(jnp.bfloat16)
        factor[h * 3 * per : (h + 1) * 3 * per, :] = jnp.dot(
            left, spread, preferred_element_type=jnp.float32
        )
    layer = lax.broadcasted_iota(jnp.int32, (LAYERS, patch), 0)
    wide = lax.broadcasted_iota(jnp.int32, (4, LANES), 1)
    lane = lax.broadcasted_iota(jnp.int32, (16, LANES), 1)
    from_left = (lane < cy) | ((lane >= edges) & (lane < edges + cy))
    from_right = ((lane >= cy) & (lane < 2 * cy)) | (lane >= edges + cy)
    from_below = (lane >= 2 * cy) & (lane < 2 * cy + cx)
    nothing = jnp.zeros((16, LANES), jnp.float32)

    for p in range(peers):
        base = p // per * 3 * per + p % per
        rows = [
            jnp.broadcast_to(factor[base + b * per : base + b * per + 1, :], (LAYERS, patch))
            for b in range(3)
        ]
        scale = jnp.where(layer < 4, rows[0], jnp.where(layer < 8, rows[1], rows[2]))
        scaled[p, 0:LAYERS, :] = scale.astype(jnp.bfloat16)

    def scale_row(i):
        for p in range(i * count_y, (i + 1) * count_y):
            part = coef_ref[:, p * patch : (p + 1) * patch] * scaled[p, 0:LAYERS, :]
            scaled[p, 0:LAYERS, :] = part
            for t in range(3):
                tile = part[:, t * LANES : (t + 1) * LANES]
                for k in range(3):
                    out_ref[place[p], 4 * t + k] = tile[4 * k : 4 * k + 4]
        row = pl.ds(i * count_y, count_y)
        found = jnp.dot(
            scaled[row].reshape(count_y * 16, patch),
            edge_ref[...],
            preferred_element_type=jnp.float32,
        )
        edge[row] = (found[:, :LANES] + found[:, LANES:]).reshape(count_y, 16, LANES)

    def join_row(i):
        for p in range(i * count_y, (i + 1) * count_y):
            j = p % count_y
            left = edge[p - count_y] if i > 0 else nothing
            right = edge[p + count_y] if i < count_x - 1 else nothing
            below = edge[p - 1] if j > 0 else nothing
            above = edge[p + 1] if j < count_y - 1 else nothing
            value = jnp.where(
                from_left, left, jnp.where(from_right, right, jnp.where(from_below, below, above))
            )
            high = value.astype(jnp.bfloat16).astype(jnp.float32)
            low = value - high
            tile = jnp.where(lane < edges, high, low).astype(jnp.bfloat16)
            for t in range(3):
                out_ref[place[p], 4 * t + 3] = tile[4 * t : 4 * t + 4]
            first = pltpu.roll(low[0:8], LANES - 2 * cy, 1)[0:4]
            second = pltpu.roll(low[0:8], LANES - 2 * cy + 2 * cx, 1)[4:8]
            third = pltpu.roll(low[8:16], (4 * cx - 2 * cy) % LANES, 1)[0:4]
            tail = jnp.where(wide < 2 * cx, first, jnp.where(wide < 4 * cx, second, third))
            tail = jnp.where(wide < 6 * cx, tail, 0.0)
            out_ref[place[p], TAIL // 4] = tail.astype(jnp.bfloat16)

    loads[1].wait()
    loads[2].wait()
    for i in range(count_x):
        scale_row(i)
        if i > 0:
            join_row(i - 1)
    join_row(count_x - 1)
    loads[3].wait()
    loads[4].wait()


def receive_table(order, cx, cy):
    parts = [depth_table(order), plane_windows(cx, cy), pick_table(cx, cy)]
    return np.concatenate([part.reshape(-1, 2 * LANES) for part in parts], axis=0)


def split(value):
    high = value.astype(jnp.bfloat16)
    return high, (value - high.astype(jnp.float32)).astype(jnp.bfloat16)


def receive_kernel(
    order, cx, cy, got_ref, right_ref, table_ref, dec_hbm, res_hbm, sum_ref,
    high_ref, low_ref, edge_ref, dec_ref, res_ref, sems,
):
    peers = got_ref.shape[0]
    groups = np.argsort([d // GROUP for d in order[::GROUP]])
    depth = peers * LAYERS
    patch = cx * cy
    count = GROUP * LAYERS
    half = patch // 2
    starts = [0, 5 * count, 10 * count] + [10 * count + half * n for n in range(1, 5)]
    starts = starts + [table_ref.shape[0]]
    table = [table_ref[a:b] for a, b in zip(starts[:-1], starts[1:])]
    deep = jnp.concatenate(table[:2], axis=1)[:, : 2 * GROUP * ROWS]
    row = lax.broadcasted_iota(jnp.int32, (count, LANES), 0)
    lane = lax.broadcasted_iota(jnp.int32, (count, LANES), 1)
    third = 2 * cx
    block = row // 4 % 3
    in_block = (lane >= block * third) & (lane < (block + 1) * third)
    for g in range(0, peers // GROUP, 2):
        both = jnp.concatenate(
            [
                got_ref[GROUP * h : GROUP * (h + 1)].reshape(GROUP * ROWS, LANES)
                for h in (groups[g], groups[g + 1])
            ],
            axis=1,
        )
        both = jnp.dot(
            deep, jnp.concatenate([both, both], axis=0), preferred_element_type=jnp.float32
        )
        for h in range(2):
            at = (g + h) * count
            for t in range(5):
                value = both[t * count : (t + 1) * count, h * LANES : (h + 1) * LANES]
                if t == 4:
                    value = jnp.where(in_block, value, 0.0)
                high, low = split(value)
                high_ref[at : at + count, t * LANES : (t + 1) * LANES] = high
                if t < 4:
                    low_ref[at : at + count, t * LANES : (t + 1) * LANES] = low

    def across(tables, refs, start):
        return lax.dot_general(
            jnp.concatenate(tables, axis=1),
            jnp.concatenate(
                [ref[:, start : start + t.shape[1]] for t, ref in zip(tables, refs)], axis=1
            ),
            (((1,), (1,)), ((), ())),
            preferred_element_type=jnp.float32,
        )

    row = lax.broadcasted_iota(jnp.int32, (cy, depth), 0)
    lane = lax.broadcasted_iota(jnp.int32, (cy, depth), 1)
    stores = []

    def store(source, target):
        stores.append(pltpu.make_async_copy(source, target, sems.at[len(stores)]))
        stores[-1].start()

    def decode(w, start):
        found = across(
            [table[2 + w], table[2 + w], table[4 + w]], [high_ref, low_ref, high_ref], start
        )
        part = pl.ds(w * cx // 2, cx // 2)
        dec_ref[part] = found.reshape(cx // 2, cy, depth)
        store(dec_ref.at[part], dec_hbm.at[part])

    def finish(x, total):
        here = dec_ref[x]
        beside = dec_ref[x - 1] if x > 0 else edge_ref[0:cy]
        beside = beside + (dec_ref[x + 1] if x < cx - 1 else edge_ref[cy : 2 * cy])
        low = edge_ref[2 * cy + x : 2 * cy + x + 1]
        high = edge_ref[2 * cy + cx + x : 2 * cy + cx + x + 1]
        beside = beside + jnp.where(row == 0, low, pltpu.roll(here, 1, 0))
        beside = beside + jnp.where(row == cy - 1, high, pltpu.roll(here, cy - 1, 0))
        beside = beside + jnp.where(lane == 0, 0.0, pltpu.roll(here, 1, 1))
        beside = beside + jnp.where(lane == depth - 1, 0.0, pltpu.roll(here, depth - 1, 1))
        left = right_ref[x] - (6.0 * here - beside)
        res_ref[x] = left
        square = left * left
        for r in range(0, cy, 8):
            for c in range(0, depth, LANES):
                total = total + square[r : r + 8, c : c + LANES]
        if x % 4 == 3:
            part = pl.ds(x - 3, 4)
            store(res_ref.at[part], res_hbm.at[part])
        return total

    total = jnp.zeros((8, LANES), jnp.float32)
    decode(0, 0)
    edge_ref[...] = across([table[6], table[6][:, :LANES]], [high_ref, low_ref], patch)
    for x in range(cx // 2 - 1):
        total = finish(x, total)
    decode(1, patch - 2 * LANES)
    for x in range(cx // 2 - 1, cx):
        total = finish(x, total)
    total = jnp.sum(total, axis=0, keepdims=True)
    sum_ref[...] = jnp.broadcast_to(total[None], sum_ref.shape)
    for copy in stores:
        copy.wait()


def finish_kernel(cells, parts_ref, rms_ref):
    total = jnp.sum(parts_ref[...].reshape(-1, LANES), axis=0, keepdims=True)
    total = jnp.sum(total, axis=1, keepdims=True)
    rms_ref[...] = jnp.sqrt(total / cells + 1e-6)


def shards(count_x, count_y, coefficients, exponents, right_side):
    peers = count_x * count_y
    cx, cy, depth = right_side.shape
    patch = cx * cy
    vmem = pl.BlockSpec(memory_space=pltpu.VMEM)
    hbm = pl.BlockSpec(memory_space=pltpu.HBM)
    order = order_of(count_x, count_y)
    tables = jnp.asarray(receive_table(order, cx, cy))
    kept = [(right_side.shape, right_side.dtype), (tables.shape, tables.dtype)]
    kept = [((peers, ROWS // 4, 4, LANES), jnp.bfloat16)] + kept
    held = sum(int(np.prod(shape)) * jnp.dtype(dtype).itemsize for shape, dtype in kept)
    near = held <= 2 << 20
    place = pltpu.VMEM if near else jax.ShapeDtypeStruct
    messages, right_side, tables = pl.pallas_call(
        functools.partial(send_kernel, order, count_x, count_y, cx, cy),
        out_shape=[place(*k) for k in kept],
        in_specs=[hbm] * 5,
        out_specs=[vmem] * 3,
        scratch_shapes=[
            pltpu.VMEM(coefficients.shape, coefficients.dtype),
            pltpu.VMEM(exponents.shape, exponents.dtype),
            pltpu.VMEM((patch, 2 * LANES), jnp.bfloat16),
            pltpu.VMEM((peers * 3, patch), jnp.float32),
            pltpu.VMEM((peers, 16, patch), jnp.bfloat16),
            pltpu.VMEM((peers, 16, LANES), jnp.float32),
            pltpu.SemaphoreType.DMA((5,)),
        ],
        compiler_params=pltpu.CompilerParams(
            vmem_limit_bytes=(64 << 20) - held - (256 << 10) if near else 48 << 20
        ),
        name="send",
    )(
        coefficients,
        exponents,
        jnp.asarray(edge_table(cx, cy)),
        right_side,
        tables,
    )
    got = exchange(messages, order)
    decoded, residual, parts = pl.pallas_call(
        functools.partial(receive_kernel, order, cx, cy),
        out_shape=(
            jax.ShapeDtypeStruct((cx, cy, depth), jnp.float32),
            jax.ShapeDtypeStruct((cx, cy, depth), jnp.float32),
            pltpu.VMEM((peers, 1, LANES), jnp.float32),
        ),
        in_specs=[vmem] * 3,
        out_specs=(hbm, hbm, vmem),
        scratch_shapes=[
            pltpu.VMEM((depth, 5 * LANES), jnp.bfloat16),
            pltpu.VMEM((depth, 4 * LANES), jnp.bfloat16),
            pltpu.VMEM((2 * cx + 2 * cy, depth), jnp.float32),
            pltpu.VMEM((cx, cy, depth), jnp.float32),
            pltpu.VMEM((cx, cy, depth), jnp.float32),
            pltpu.SemaphoreType.DMA((2 + cx // 4,)),
        ],
        compiler_params=pltpu.CompilerParams(vmem_limit_bytes=(12 << 20) * peers // 32),
        name="receive",
    )(got, right_side, tables)
    parts = exchange(parts, order)
    rms = pl.pallas_call(
        functools.partial(finish_kernel, patch * depth * peers),
        out_shape=jax.ShapeDtypeStruct((1, 1), jnp.float32),
        in_specs=[vmem],
        out_specs=vmem,
        compiler_params=pltpu.CompilerParams(vmem_limit_bytes=1 << 20),
        name="finish",
    )(parts)
    return (decoded, residual, rms.reshape(()))


def solution(mesh):
    return jax.shard_map(
        functools.partial(shards, mesh.shape["px"], mesh.shape["py"]),
        mesh=mesh,
        in_specs=(P(AXES, None), P(AXES, None), P("px", "py", None)),
        out_specs=(P("px", "py", None), P("px", "py", None), P()),
        check_vma=False,
    )
```
